32 devices in a mesh: part: 2 (over x), col: 4 (over z), row: 4 (over y, core).
Axes of the slice: x: 2, y: 2, z: 4, core: 2. Of those that a mesh axis runs over, the one named last changes fastest.
Arguments:
- matrix: float32 [32768, 4, 48], P(('part', 'row'), 'col'), parts along dimension 0
Outputs:
- output 1: float32 [32768, 4, 48], P(('part', 'row'), 'col'), parts along dimension 0
- output 2: float32 [8, 48], P('part'), parts along dimension 0
- output 3: float32 [8, 48, 48], P('part'), parts along dimension 0
- output 4: float32 [32768, 192], P(('part', 'row')), parts along dimension 0
There are 2 independent parts. The reference program is written for one: setup_inputs(seed, part) draws one part's arguments, and reference() takes and returns one part's arrays. A program takes and returns all parts, laid end to end along the dimension named above; each array names one.
All inputs are finite; a program needn't handle non-finite values.
Results may differ from the reference program's by a relative error of at most 0.001.
Values sent between devices are 32-bit elements.
A program may use at most 1 GiB of HBM per device.

```python
import jax
import jax.numpy as jnp
from jax import lax

MAT_ROWS = 16384
BLOCK_COLS = 48
PROC_COLS = 4
PANELS_DEV = 1
NUM_PANELS = PANELS_DEV * PROC_COLS
NUM_COLS = NUM_PANELS * BLOCK_COLS
HIGHEST = lax.Precision.HIGHEST


def matmul(lhs_mat, rhs_mat):
    return jnp.dot(lhs_mat, rhs_mat, precision=HIGHEST, preferred_element_type=jnp.float32)


def entry_to_logical(entry_mat):
    return entry_mat.reshape(MAT_ROWS, PROC_COLS, PANELS_DEV, BLOCK_COLS).transpose(0, 2, 1, 3).reshape(MAT_ROWS, NUM_COLS)


def logical_to_entry(logical):
    return logical.reshape(MAT_ROWS, PANELS_DEV, PROC_COLS, BLOCK_COLS).transpose(0, 2, 1, 3).reshape(MAT_ROWS, NUM_PANELS, BLOCK_COLS)


def setup_inputs(seed: int = 0, part: int = 0) -> dict:
    part_key = jax.random.fold_in(jax.random.key(seed), part)
    key_base, key_block, key_sign = jax.random.split(part_key, 3)
    row_ids = jnp.arange(MAT_ROWS)[:, None]
    col_ids = jnp.arange(NUM_COLS)[None, :]
    base_noise = jax.random.normal(key_base, (MAT_ROWS, NUM_COLS), jnp.float32)
    block_noise = jax.random.normal(key_block, (MAT_ROWS, NUM_COLS), jnp.float32)
    diag_signs = (2 * jax.random.randint(key_sign, (1, NUM_COLS), 0, 2) - 1).astype(jnp.float32)
    in_block = (row_ids // BLOCK_COLS == col_ids // BLOCK_COLS) & (row_ids > col_ids)
    block_scale = 0.3 * (MAT_ROWS / BLOCK_COLS) ** 0.5
    diag_scale = 0.5 * MAT_ROWS ** 0.5
    logical = base_noise + jnp.where(in_block, block_scale * block_noise, 0.0)
    logical = logical + jnp.where(row_ids == col_ids, diag_scale * diag_signs, 0.0)
    return {"matrix": logical_to_entry(logical)}


def factor_panel(panel_in, diag0):
    row_ids = jnp.arange(MAT_ROWS)
    col_ids = jnp.arange(BLOCK_COLS)

    def column_step(col_step, carried):
        panel_work, refl_vecs, tau_vec = carried
        diag_row = diag0 + col_step
        column = lax.dynamic_index_in_dim(panel_work, col_step, axis=1, keepdims=False)
        x_col = jnp.where(row_ids >= diag_row, column, 0.0)
        alpha_val = lax.dynamic_index_in_dim(column, diag_row, keepdims=False)
        col_norm = jnp.sqrt(jnp.sum(x_col * x_col))
        beta_val = jnp.where(alpha_val >= 0, -col_norm, col_norm)
        tau_step = (beta_val - alpha_val) / beta_val
        at_diag = row_ids == diag_row
        reflector = jnp.where(row_ids > diag_row, x_col / (alpha_val - beta_val), jnp.where(at_diag, 1.0, 0.0))
        v_dots = jnp.where(col_ids > col_step, matmul(reflector, panel_work), 0.0)
        panel_work = panel_work - tau_step * reflector[:, None] * v_dots[None, :]
        new_col = jnp.where(row_ids < diag_row, column, jnp.where(at_diag, beta_val, reflector))
        is_col = col_ids == col_step
        panel_work = jnp.where(is_col[None, :], new_col[:, None], panel_work)
        refl_vecs = jnp.where(is_col[None, :], reflector[:, None], refl_vecs)
        tau_vec = jnp.where(is_col, tau_step, tau_vec)
        return panel_work, refl_vecs, tau_vec

    init_carry = (panel_in, jnp.zeros_like(panel_in), jnp.zeros((BLOCK_COLS,), jnp.float32))
    return lax.fori_loop(0, BLOCK_COLS, column_step, init_carry)


def build_tfac(refl_vecs, tau_vec):
    col_ids = jnp.arange(BLOCK_COLS)
    gram_mat = matmul(refl_vecs.T, refl_vecs)

    def t_step(col_step, t_fac):
        g_col = jnp.where(col_ids < col_step, lax.dynamic_index_in_dim(gram_mat, col_step, axis=1, keepdims=False), 0.0)
        tau_step = tau_vec[col_step]
        new_col = jnp.where(col_ids == col_step, tau_step, -tau_step * matmul(t_fac, g_col))
        return jnp.where(col_ids[None, :] == col_step, new_col[:, None], t_fac)

    return lax.fori_loop(0, BLOCK_COLS, t_step, jnp.zeros((BLOCK_COLS, BLOCK_COLS), jnp.float32))


def reference(matrix):
    col_pos = jnp.arange(NUM_COLS)

    def panel_step(work_mat, panel_idx):
        first_col = panel_idx * BLOCK_COLS
        panel_in = lax.dynamic_slice_in_dim(work_mat, first_col, BLOCK_COLS, axis=1)
        panel_out, refl_vecs, tau_vec = factor_panel(panel_in, first_col)
        t_fac = build_tfac(refl_vecs, tau_vec)
        work_mat = lax.dynamic_update_slice_in_dim(work_mat, panel_out, first_col, axis=1)
        proj_sum = matmul(t_fac.T, matmul(refl_vecs.T, work_mat))
        proj_sum = jnp.where(col_pos[None, :] >= first_col + BLOCK_COLS, proj_sum, 0.0)
        work_mat = work_mat - matmul(refl_vecs, proj_sum)
        return work_mat, (refl_vecs, t_fac)

    scanned = lax.scan(panel_step, entry_to_logical(matrix), jnp.arange(NUM_PANELS))
    work_mat = scanned[0]
    all_vecs = scanned[1][0]
    all_tfac = scanned[1][1]
    q_init = (jnp.arange(MAT_ROWS)[:, None] == col_pos[None, :]).astype(jnp.float32)

    def q_step(q_cur, panel_pair):
        refl_vecs = panel_pair[0]
        t_fac = panel_pair[1]
        inner_prod = matmul(t_fac, matmul(refl_vecs.T, q_cur))
        return q_cur - matmul(refl_vecs, inner_prod), None

    q_mat = lax.scan(q_step, q_init, (all_vecs, all_tfac), reverse=True)[0]
    tau_vals = jnp.diagonal(all_tfac, axis1=1, axis2=2)
    return logical_to_entry(work_mat), tau_vals, all_tfac, q_mat
```

```python
import functools
import jax
import jax.numpy as jnp
from jax import lax
from jax.experimental import pallas as pl
from jax.experimental.pallas import tpu as pltpu
from jax.sharding import PartitionSpec as P

HIGHEST = lax.Precision.HIGHEST
MESH = pl.DeviceIdType.MESH
W = 48
NP = 4
N = W * NP
NC = 8
WIN = 4
F32 = jnp.float32
SUM_BOUND = 6144.0


def mm(a, b):
    return lax.dot_general(a, b, (((1,), (0,)), ((), ())), precision=HIGHEST, preferred_element_type=F32)


def mm_nt(a, b):
    return lax.dot_general(a, b, (((1,), (1,)), ((), ())), precision=HIGHEST, preferred_element_type=F32)


def iota(shape, dim):
    return lax.broadcasted_iota(jnp.int32, shape, dim)


def roll(x, shift):
    shift = shift % x.shape[1]
    return x if shift == 0 else pltpu.roll(x, shift, 1)


def widen(x, lanes):
    return jnp.concatenate([x, jnp.zeros((x.shape[0], lanes - x.shape[1]), F32)], axis=1)


def chain(limit, xc_ref, hn_ref, vt_ref, fr_ref, rn_ref, td_ref):
    ng = W // 8
    sub = iota((8, 128), 0)
    lane = iota((8, 128), 1)
    live0 = lane < limit
    live1 = lane + 128 < limit
    xs0 = [xc_ref[8 * s:8 * s + 8, 0:128] for s in range(ng)]
    xs1 = [xc_ref[8 * s:8 * s + 8, 128:256] for s in range(ng)]
    hs = [hn_ref[8 * s:8 * s + 8, :] for s in range(ng)]

    def bcast_sub(x, u):
        return jnp.broadcast_to(x[u:u + 1, :], (8, 128))

    def bcast_col(x, k):
        return jnp.broadcast_to(x[:, k:k + 1], (8, 128))

    def columns(k):
        return ({s: bcast_col(hs[s], k) for s in range(k // 8, ng)}, {s: bcast_col(xs0[s], k) for s in range(0, ng)})

    window = {k: columns(k) for k in range(WIN)}
    for k in range(W):
        s0, u = k // 8, k % 8
        ch, cx = window.pop(k)
        hkk = bcast_sub(ch[s0], u)
        alpha = bcast_sub(cx[s0], u)
        inv_norm = lax.rsqrt(hkk)
        inv_beta = jnp.where(alpha >= 0, -inv_norm, inv_norm)
        beta = hkk * inv_beta
        inv = 1.0 / (alpha - beta)
        tau = (beta - alpha) * inv_beta
        below = sub > u
        rc, wc = {}, {}
        for s in range(s0, ng):
            r = ch[s] * inv_beta
            w = cx[s] - r
            rc[s] = jnp.where(below, r, 0.0) if s == s0 else r
            wc[s] = jnp.where(below, w, 0.0) if s == s0 else w
        r_of = {}
        for m in range(k + 1, min(k + WIN, W)):
            mh, mx = window[m]
            r_m = bcast_sub(rc[m // 8], m % 8)
            v_m = bcast_sub(mx[s0], u) * inv
            for s in range(m // 8, ng):
                mh[s] = mh[s] - rc[s] * r_m
            for s in range(s0, ng):
                mx[s] = mx[s] - wc[s] * v_m
        hrow = bcast_sub(hs[s0], u) * inv_beta
        x0 = bcast_sub(xs0[s0], u)
        x1 = bcast_sub(xs1[s0], u)
        s0v = x0 * inv
        v0 = jnp.where(live0 & (lane > k), s0v, jnp.where(lane == k, 1.0, 0.0))
        v1 = jnp.where(live1, x1 * inv, 0.0)
        vt_ref[k:k + 1, 0:128] = v0[0:1, :]
        vt_ref[k:k + 1, 128:256] = v1[0:1, :]
        fr_ref[k:k + 1, 0:128] = jnp.where(live0 & (lane > k), s0v, jnp.where(lane == k, beta, x0))[0:1, :]
        fr_ref[k:k + 1, 128:256] = jnp.where(live1, v1, x1)[0:1, :]
        rn_ref[k:k + 1, :] = hrow[0:1, :]
        td_ref[k:k + 1, :] = jnp.where(lane == k, tau, 0.0)[0:1, :]
        for s in range(s0, ng):
            hs[s] = hs[s] - rc[s] * hrow
            xs0[s] = xs0[s] - wc[s] * v0
            xs1[s] = xs1[s] - wc[s] * v1
        if k + WIN < W:
            window[k + WIN] = columns(k + WIN)


def load_panel(g, refs):
    xt, e1, e2, rts, wts, rinvd, rnat, kvt, xc_ref, hn_ref, dvec = (
        refs["xt"], refs["e1"], refs["e2"], refs["rts"], refs["wts"], refs["rinvd"], refs["rnat"], refs["kv"], refs["xc"], refs["hn"], refs["dvec"])
    x = xt[g]
    lane = iota((W, 256), 1)
    row = iota((W, 256), 0)
    diag = jnp.sum(jnp.where(lane == row + N, x, 0.0), axis=0, keepdims=True)
    dvec[0:1, :] = dvec[0:1, :] + roll(diag, 64 + W * g)
    gram = roll(x, 64)[:, 0:128]
    lane1 = lane[:, 0:128]
    row1 = row[:, 0:128]
    x = jnp.where(lane >= N, jnp.where(lane == row + N, 1.0, 0.0), x)
    hgg = gram[:, 0:W]
    for h in range(g):
        if g - h == 1:
            hgh = e1[g][:, 0:W]
        elif g - h == 2:
            hgh = roll(e1[g], 80)[:, 0:W]
        else:
            hgh = e2[0][:, 0:W] + e2[1][:, 0:W]
        for q in range(h):
            hgh = hgh - mm_nt(rts[g, q], rts[h, q])
        rt = mm_nt(hgh, rinvd[h])
        d = hgh - mm(x[:, 0:W], rnat[h])
        both = mm(d, kvt[h])
        x = roll(x - both[:, 0:256], 256 - W)
        hgg = hgg - mm_nt(rt, rt)
        rts[g, h] = rt
        wts[g, h] = both[:, 256:256 + W]
    xc_ref[...] = x
    hn_ref[...] = jnp.where(lane1 < W, widen(hgg, 128), jnp.where(lane1 == row1 + 64, 1.0, 0.0))


def close_panel(g, refs):
    vt = refs["vt"][...]
    fr = refs["fr"][...]
    rn = refs["rn"][...]
    td = refs["td"][...]
    lane = iota((W, 256), 1)
    lane1 = iota((W, 128), 1)
    row1 = iota((W, 128), 0)
    sq_lane = iota((W, W), 1)
    sq_row = iota((W, W), 0)
    refs["ftop"][g] = roll(fr, W * g)
    mt = roll(vt, 64 + W * g)[:, 0:W]
    v = jnp.where(lane < N - W * g, vt, 0.0)
    rnat = jnp.where((lane1 >= row1) & (lane1 < W), rn, 0.0)[:, 0:W]
    rinvt = roll(rn, 64)[:, 0:W]
    rinvt = jnp.where(sq_lane <= sq_row, rinvt, 0.0)
    mt = jnp.where(sq_lane <= sq_row, mt, 0.0)
    refs["rnat"][g] = rnat
    refs["rinvd"][g] = rinvt
    s = -mm(v[:, 0:W], mm_nt(rnat, mt))
    t = td[:, 0:W]
    refs["tau"][g:g + 1, :] = jnp.sum(td, axis=0, keepdims=True)[:, 0:W]
    size = 1
    while size < W:
        pair = (sq_row // (2 * size) == sq_lane // (2 * size)) & (sq_row // size < sq_lane // size)
        t = t - mm(mm(t, jnp.where(pair, s, 0.0)), t)
        size *= 2
    refs["t"][g] = t
    if g + 1 < NP:
        kmat = lax.dot_general(mt, t, (((0,), (0,)), ((), ())), precision=HIGHEST, preferred_element_type=F32)
        refs["kv"][g, :, 0:256] = mm(kmat, v)
        refs["kv"][g, :, 256:384] = widen(kmat, 128)
    lr = roll(widen(rinvt, 256), W * g)
    lc = roll(widen(mt, 256), W * g)
    if g:
        rcat = sum(roll(widen(refs["rts"][g, h], 256), W * h) for h in range(g))
        wcat = sum(roll(widen(refs["wts"][g, h], 256), W * h) for h in range(g))
        lr = lr - mm(mm(rinvt, rcat)[:, 0:N], refs["lr"][...])
        lc = lc - mm(mm(mt, wcat)[:, 0:N], refs["lc"][...])
    refs["lr"][W * g:W * g + W, :] = lr
    refs["lc"][W * g:W * g + W, :] = lc


def fused_kernel(a_hbm, q_hbm, f_hbm, tau_ref, t_ref, flag_ref, panels, xt, e1, e2, x0s, x1s, x2s, x3s, g1s, g1r, g2s, g2r, h1s, h1r, h2s, h2r,
                 rts, wts, rinvd, rnat, kvt, xc, hn, dvec, vt, fr, rn, td, ftop, lr, lc, lhs, q_stage, f_stage,
                 load_sem, send_sem, bulk_sem, ex_send, ex_recv, e0_send, e0_recv, e1_send, e1_recv, e2_send, e2_recv, q_sem, f_sem):
    refs = dict(xt=xt, e1=e1, e2=e2, rts=rts, wts=wts, rinvd=rinvd, rnat=rnat, kv=kvt, xc=xc, hn=hn, dvec=dvec,
                vt=vt, fr=fr, rn=rn, td=td, ftop=ftop, lr=lr, lc=lc, tau=tau_ref, t=t_ref)
    part = lax.axis_index("part")
    c = lax.axis_index("col")
    r = lax.axis_index("row")
    width = panels.shape[3]
    twin = r + 1 - 2 * lax.rem(r, 2)
    across = lax.rem(r + 2, 4)

    def at(col, row):
        return (part, col, row)

    for q in range(NC):
        pltpu.make_async_copy(a_hbm.at[:, pl.ds(q * width, width)], panels.at[c, q], load_sem.at[q]).start()

    barrier = pltpu.get_barrier_semaphore()
    for s in range(1, NP):
        pl.semaphore_signal(barrier, inc=1, device_id=at(lax.rem(c + s, NP), r), device_id_type=MESH)
    pl.semaphore_signal(barrier, inc=1, device_id=at(c, twin), device_id_type=MESH)
    pl.semaphore_signal(barrier, inc=1, device_id=at(c, across), device_id_type=MESH)
    pl.semaphore_wait(barrier, NP + 1)

    lr[...] = jnp.zeros_like(lr)
    lc[...] = jnp.zeros_like(lc)
    dvec[...] = jnp.zeros_like(dvec)
    e2[...] = jnp.zeros_like(e2)

    order_l = list(range(NC))
    order_r = list(range(NC // 2, NC)) + list(range(NC // 2))

    def bulk(side, g, q):
        other = c - 1 if side == 0 else c + 1
        return pltpu.make_async_remote_copy(
            src_ref=panels.at[g, q], dst_ref=panels.at[g, q], send_sem=send_sem.at[side, g, q], recv_sem=bulk_sem.at[g, q],
            device_id=at(other, r), device_id_type=MESH)

    def start_own(i):
        @pl.when(c >= 1)
        def _():
            bulk(0, c, order_l[i]).start()

        @pl.when(c <= NP - 2)
        def _():
            bulk(1, c, order_r[i]).start()

    def arrive(dist, i):
        @pl.when(c + dist <= NP - 1)
        def _():
            bulk(0, c + dist, order_l[i]).wait_recv()

        @pl.when(c - dist >= 0)
        def _():
            bulk(1, c - dist, order_r[i]).wait_recv()

    def forward(dist, i):
        @pl.when((c + dist <= NP - 1) & (c >= 1))
        def _():
            bulk(0, c + dist, order_l[i]).start()

        @pl.when((c - dist >= 0) & (c <= NP - 2))
        def _():
            bulk(1, c - dist, order_r[i]).start()

    def row_sum(e, mine, got1, half, got2, out, slot):
        first = pltpu.make_async_remote_copy(mine, got1, ex_send.at[e, 0], ex_recv.at[e, 0], device_id=at(c, twin), device_id_type=MESH)
        first.start()
        first.wait()
        half[...] = mine[...] + got1[...]
        second = pltpu.make_async_remote_copy(half, got2, ex_send.at[e, 1], ex_recv.at[e, 1], device_id=at(c, across), device_id_type=MESH)
        second.start()
        second.wait()
        out[slot] = half[...] + got2[...]

    def shared(ref, slot, ssem, rsem, sslot, s, rslot):
        return pltpu.make_async_remote_copy(ref.at[slot], ref.at[slot], ssem.at[sslot], rsem.at[rslot],
                                            device_id=at(lax.rem(c + s, NP), r), device_id_type=MESH)

    def chunk_cols(g, q):
        return panels[g, q]

    for q in range(NC):
        pltpu.make_async_copy(a_hbm.at[:, pl.ds(q * width, width)], panels.at[c, q], load_sem.at[q]).wait()
    head = 3
    for i in range(head):
        start_own(i)
    gram = jnp.zeros((W, W), F32)
    for q in range(NC):
        blk = chunk_cols(c, q)
        gram = gram + mm_nt(blk, blk)
    lane = iota((W, 256), 1)
    top = jnp.where((lane < N) & (r == 0), panels[c, 0, :, 0:256], 0.0)
    x0s[...] = top + roll(widen(gram, 256), N)
    row_sum(0, x0s, x1s, x2s, x3s, xt, c)
    for s in range(1, NP):
        shared(xt, c, e0_send, e0_recv, s - 1, s, c).start()
    for i in range(head, NC):
        start_own(i)

    def wait_e0(g):
        @pl.when(c != g)
        def _():
            shared(xt, g, e0_send, e0_recv, 0, 1, g).wait_recv()

    def wait_e1(g):
        @pl.when(c != g - 1)
        def _():
            shared(e1, g, e1_send, e1_recv, 0, 1, g).wait_recv()

    def wait_e2(i):
        @pl.when(c != i + 1)
        def _():
            shared(e2, i, e2_send, e2_recv, 0, 1, i).wait_recv()

    def before(g):
        if g == 0:
            wait_e0(0)
        if g == 1:
            for i in range(NC):
                arrive(1, i)
                if i < head:
                    forward(1, i)

            @pl.when(c <= NP - 2)
            def _():
                left = jnp.maximum(c - 1, 0)
                acc = jnp.zeros((W, 2 * W), F32)
                for q in range(NC):
                    pair = jnp.concatenate([chunk_cols(c, q), chunk_cols(left, q)], axis=0)
                    acc = acc + mm_nt(chunk_cols(c + 1, q), pair)
                g1s[...] = widen(acc, 128)
                row_sum(1, g1s, g1r, g2s, g2r, e1, c + 1)
                for s in range(1, NP):
                    shared(e1, c + 1, e1_send, e1_recv, s - 1, s, c + 1).start()
            for i in range(head, NC):
                forward(1, i)
            wait_e0(1)
            wait_e1(1)
        if g == 2:
            half = NC // 2
            for i in range(half):
                arrive(2, i)
                if i < 1:
                    forward(2, i)

            @pl.when((c >= 1) & (c <= 2))
            def _():
                base = (c - 1) * half
                acc = jnp.zeros((W, W), F32)
                for i in range(half):
                    acc = acc + mm_nt(chunk_cols(3, base + i), chunk_cols(0, base + i))
                h1s[...] = widen(acc, 128)
                row_sum(2, h1s, h1r, h2s, h2r, e2, c - 1)
                for s in range(1, NP):
                    shared(e2, c - 1, e2_send, e2_recv, s - 1, s, c - 1).start()
            for i in range(1, half):
                forward(2, i)
            wait_e0(2)
            wait_e1(2)
        if g == 3:
            for i in range(NC // 2, NC):
                arrive(2, i)
                forward(2, i)
            wait_e0(3)
            wait_e1(3)
            wait_e2(0)
            wait_e2(1)

    def panel_step(g, carry):
        for s in range(NP):
            @pl.when(g == s)
            def _():
                before(s)
                load_panel(s, refs)
        chain(256 - W * g, xc, hn, vt, fr, rn, td)
        for s in range(NP):
            @pl.when(g == s)
            def _():
                close_panel(s, refs)
        return carry

    lax.fori_loop(0, NP, panel_step, 0)

    dv = dvec[0:1, 0:N]
    lr_all = lr[...][:, 0:N]
    lc_all = lc[...][:, 0:N]
    good = ((jnp.sum(lr_all * lr_all * dv) <= SUM_BOUND) & (jnp.sum(lc_all * lc_all * dv) <= SUM_BOUND)
            & (jnp.min(dv) > 1e-18) & (jnp.max(dv) < 1e30))
    flag_ref[...] = jnp.zeros((8, 128), F32) + jnp.where(good, 0.0, 1.0)

    lhs[0:N, :] = lr[...]
    lhs[N:N + W, :] = lc[pl.ds(pl.multiple_of(c * W, W), W), :]
    ftop_c = ftop[c]

    def out_copies(slot, q):
        cols = pl.ds(pl.multiple_of(q * width, width), width)
        return (pltpu.make_async_copy(q_stage.at[slot], q_hbm.at[:, cols], q_sem.at[slot]),
                pltpu.make_async_copy(f_stage.at[slot], f_hbm.at[:, cols], f_sem.at[slot]))

    def out_step(i, carry):
        q = lax.rem(i + jnp.where(c >= 2, NC // 2, 0), NC)
        slot = lax.rem(i, 2)

        @pl.when(c == 0)
        def _():
            bulk(0, 3, q).wait_recv()

        @pl.when(c == NP - 1)
        def _():
            bulk(1, 0, q).wait_recv()

        @pl.when(i >= 2)
        def _():
            for cp in out_copies(slot, q):
                cp.wait()
        rhs = jnp.concatenate([panels[g, q] for g in range(NP)], axis=0)
        prod = mm(lhs[:, 0:N], rhs)
        q_stage[slot] = prod[0:N]
        f_stage[slot] = prod[N:N + W]

        @pl.when((q == 0) & (r == 0))
        def _():
            keep = iota((W, 256), 1) < N
            f_stage[slot, :, 0:256] = jnp.where(keep, ftop_c, prod[N:N + W, 0:256])
        for cp in out_copies(slot, q):
            cp.start()
        return carry

    lax.fori_loop(0, NC, out_step, 0)
    for slot in range(2):
        for cp in out_copies(slot, 0):
            cp.wait()

    for i in range(NC):
        @pl.when(c >= 1)
        def _():
            for s in range(NP):
                @pl.when(c <= s)
                def _():
                    bulk(0, s, i).wait_send()

        @pl.when(c <= NP - 2)
        def _():
            for s in range(NP):
                @pl.when(c >= s)
                def _():
                    bulk(1, s, i).wait_send()
    for s in range(1, NP):
        shared(xt, c, e0_send, e0_recv, s - 1, s, c).wait_send()

        @pl.when(c <= NP - 2)
        def _():
            shared(e1, c + 1, e1_send, e1_recv, s - 1, s, c + 1).wait_send()

        @pl.when((c >= 1) & (c <= 2))
        def _():
            shared(e2, c - 1, e2_send, e2_recv, s - 1, s, c - 1).wait_send()


def fused_qr(a_t):
    rows = a_t.shape[1]
    width = rows // NC
    vm = lambda *shape: pltpu.VMEM(shape, F32)
    dma = lambda *shape: pltpu.SemaphoreType.DMA(shape)
    out = lambda *shape: jax.ShapeDtypeStruct(shape, F32)
    hbm = pl.BlockSpec(memory_space=pl.ANY)
    vmem = pl.BlockSpec(memory_space=pltpu.VMEM)
    scratch = [vm(NP, NC, W, width), vm(NP, W, 256), vm(NP, W, 128), vm(2, W, 128), vm(W, 256), vm(W, 256), vm(W, 256)]
    scratch += [vm(W, 256)]
    scratch += [vm(W, 128)] * 8
    scratch += [vm(NP, 3, W, W), vm(NP, 3, W, W), vm(NP, W, W), vm(NP, W, W), vm(3, W, 384), vm(W, 256), vm(W, 128), vm(8, 256),
                vm(W, 256), vm(W, 256), vm(W, 128), vm(W, 128), vm(NP, W, 256), vm(N, 256), vm(N, 256), vm(N + W, 256),
                vm(2, N, width), vm(2, W, width)]
    scratch += [dma(NC), dma(2, NP, NC), dma(NP, NC), dma(3, 2), dma(3, 2), dma(3), dma(NP), dma(3), dma(NP), dma(3), dma(2), dma(2), dma(2)]
    return pl.pallas_call(
        fused_kernel,
        name="fused_qr",
        out_shape=(out(N, rows), out(W, rows), out(NP, W), out(NP, W, W), out(8, 128)),
        in_specs=[hbm],
        out_specs=(hbm, hbm, vmem, vmem, vmem),
        scratch_shapes=scratch,
        compiler_params=pltpu.CompilerParams(collective_id=0, has_side_effects=True, vmem_limit_bytes=32 * 1024 * 1024),
    )(a_t)


def dot_high(lhs_mat, rhs_mat):
    return jnp.dot(lhs_mat, rhs_mat, precision=HIGHEST, preferred_element_type=jnp.float32)


def contract(einsum_form, lhs_mat, rhs_mat):
    return jnp.einsum(einsum_form, lhs_mat, rhs_mat, precision=HIGHEST, preferred_element_type=jnp.float32)


def factor_panel(panel_in, row_start, diag0, reduce_rows):
    rows_loc, panel_width = panel_in.shape
    global_rows = row_start + jnp.arange(rows_loc)
    col_ids = jnp.arange(panel_width)

    def column_step(col_step, carried):
        panel_work, refl_vecs, tau_vec = carried
        diag_row = diag0 + col_step
        column = lax.dynamic_index_in_dim(panel_work, col_step, axis=1, keepdims=False)
        x_col = jnp.where(global_rows >= diag_row, column, 0.0)
        local_row = diag_row - row_start
        holds_diag = (local_row >= 0) & (local_row < rows_loc)
        diag_row_vals = lax.dynamic_index_in_dim(panel_work, jnp.clip(local_row, 0, rows_loc - 1), axis=0, keepdims=False)
        diag_piece = jnp.where(holds_diag, diag_row_vals, 0.0)
        summed = reduce_rows(jnp.stack([dot_high(x_col, panel_work), diag_piece]))
        x_dots = summed[0]
        diag_vals = summed[1]
        alpha_val = diag_vals[col_step]
        col_norm = jnp.sqrt(x_dots[col_step])
        beta_val = jnp.where(alpha_val >= 0, -col_norm, col_norm)
        tau_step = (beta_val - alpha_val) / beta_val
        inv_scale = 1.0 / (alpha_val - beta_val)
        at_diag = global_rows == diag_row
        reflector = jnp.where(global_rows > diag_row, x_col * inv_scale, jnp.where(at_diag, 1.0, 0.0))
        v_dots = jnp.where(col_ids > col_step, inv_scale * (x_dots - alpha_val * diag_vals) + diag_vals, 0.0)
        panel_work = panel_work - tau_step * reflector[:, None] * v_dots[None, :]
        new_col = jnp.where(global_rows < diag_row, column, jnp.where(at_diag, beta_val, reflector))
        is_col = col_ids == col_step
        panel_work = jnp.where(is_col[None, :], new_col[:, None], panel_work)
        refl_vecs = jnp.where(is_col[None, :], reflector[:, None], refl_vecs)
        tau_vec = jnp.where(is_col, tau_step, tau_vec)
        return panel_work, refl_vecs, tau_vec

    init_carry = (panel_in, jnp.zeros_like(panel_in), jnp.zeros((panel_width,), jnp.float32))
    return lax.fori_loop(0, panel_width, column_step, init_carry)


def build_tfac(refl_vecs, tau_vec, reduce_rows):
    panel_width = tau_vec.shape[0]
    col_ids = jnp.arange(panel_width)
    gram_mat = reduce_rows(contract("rk,rl->kl", refl_vecs, refl_vecs))

    def t_step(col_step, t_fac):
        g_col = jnp.where(col_ids < col_step, lax.dynamic_index_in_dim(gram_mat, col_step, axis=1, keepdims=False), 0.0)
        tau_step = tau_vec[col_step]
        new_col = jnp.where(col_ids == col_step, tau_step, -tau_step * dot_high(t_fac, g_col))
        return jnp.where(col_ids[None, :] == col_step, new_col[:, None], t_fac)

    return lax.fori_loop(0, panel_width, t_step, jnp.zeros((panel_width, panel_width), jnp.float32))


def careful_program(proc_cols):
    sum_rows = functools.partial(lax.psum, axis_name="row")

    def local_program(a_loc):
        rows_loc, panels_loc, panel_width = a_loc.shape
        num_panels = panels_loc * proc_cols
        col_idx = lax.axis_index("col")
        row_start = lax.axis_index("row") * rows_loc
        global_rows = row_start + jnp.arange(rows_loc)
        panel_ids = jnp.arange(panels_loc) * proc_cols + col_idx

        def panel_step(panel_idx, carried):
            a_work, all_vecs, all_tfac = carried
            slot_idx = panel_idx // proc_cols
            is_owner = col_idx == panel_idx % proc_cols
            old_panel = lax.dynamic_index_in_dim(a_work, slot_idx, axis=1, keepdims=False)
            new_panel, refl_vecs, tau_vec = factor_panel(old_panel, row_start, panel_idx * panel_width, sum_rows)
            t_fac = build_tfac(refl_vecs, tau_vec, sum_rows)
            refl_vecs, t_fac = lax.psum((jnp.where(is_owner, refl_vecs, 0.0), jnp.where(is_owner, t_fac, 0.0)), "col")
            a_work = lax.dynamic_update_index_in_dim(a_work, jnp.where(is_owner, new_panel, old_panel), slot_idx, axis=1)
            proj_sum = sum_rows(contract("rk,rsj->ksj", refl_vecs, a_work))
            w_block = contract("kl,ksj->lsj", t_fac, proj_sum)
            w_block = jnp.where((panel_ids > panel_idx)[None, :, None], w_block, 0.0)
            a_work = a_work - contract("rl,lsj->rsj", refl_vecs, w_block)
            all_vecs = lax.dynamic_update_index_in_dim(all_vecs, refl_vecs, panel_idx, axis=0)
            all_tfac = lax.dynamic_update_index_in_dim(all_tfac, t_fac, panel_idx, axis=0)
            return a_work, all_vecs, all_tfac

        init_carry = (a_loc, jnp.zeros((num_panels, rows_loc, panel_width), jnp.float32), jnp.zeros((num_panels, panel_width, panel_width), jnp.float32))
        a_work, all_vecs, all_tfac = lax.fori_loop(0, num_panels, panel_step, init_carry)
        logical_cols = panel_ids[:, None] * panel_width + jnp.arange(panel_width)[None, :]
        q_init = (global_rows[:, None, None] == logical_cols[None, :, :]).astype(jnp.float32)

        def q_step(back_step, q_local):
            panel_idx = num_panels - 1 - back_step
            refl_vecs = lax.dynamic_index_in_dim(all_vecs, panel_idx, keepdims=False)
            t_fac = lax.dynamic_index_in_dim(all_tfac, panel_idx, keepdims=False)
            proj_sum = sum_rows(contract("rk,rsj->ksj", refl_vecs, q_local))
            w_block = contract("kl,lsj->ksj", t_fac, proj_sum)
            return q_local - contract("rk,ksj->rsj", refl_vecs, w_block)

        q_local = lax.fori_loop(0, num_panels, q_step, q_init)
        gathered = lax.all_gather(q_local, "col")
        q_rows = gathered.transpose(1, 2, 0, 3).reshape(rows_loc, num_panels * panel_width)
        tau_vals = jnp.diagonal(all_tfac, axis1=1, axis2=2)
        return a_work, tau_vals, all_tfac, q_rows

    return local_program


def solution(mesh):
    careful = careful_program(mesh.shape["col"])

    def local_program(a_loc):
        rows_loc = a_loc.shape[0]
        q_t, f_t, tau_vals, t_fac, flag = fused_qr(a_loc.reshape(rows_loc, W).T)

        def again(state):
            factored, tau_new, t_new, q_new = careful(a_loc)
            return jnp.float32(0.0), factored, tau_new, t_new, q_new

        state = (flag[0, 0], f_t.T.reshape(rows_loc, 1, W), tau_vals, t_fac, q_t.T)
        return lax.while_loop(lambda s: s[0] > 0.5, again, state)[1:]

    spec_rows = P(("part", "row"), "col", None)
    out_specs = (spec_rows, P("part", None), P("part", None, None), P(("part", "row"), None))
    return jax.shard_map(local_program, mesh=mesh, in_specs=(spec_rows,), out_specs=out_specs, check_vma=False)
```

```python
import functools
import jax
import jax.numpy as jnp
from jax import lax
from jax.experimental import pallas as pl
from jax.experimental.pallas import tpu as pltpu
from jax.sharding import PartitionSpec as P

HIGHEST = lax.Precision.HIGHEST
MESH = pl.DeviceIdType.MESH
W = 48
NP = 4
N = W * NP
NC = 8
WIN = 4
F32 = jnp.float32
SUM_BOUND = 6144.0
STEPS = 8
AUX_TOP = N + W
AUX_T = AUX_TOP + W
AUX_TAU = AUX_T + N
AUX_MODE = AUX_TAU + 8
AUX_ROWS = AUX_MODE + 8


def mm(a, b):
    return lax.dot_general(a, b, (((1,), (0,)), ((), ())), precision=HIGHEST, preferred_element_type=F32)


def mm_nt(a, b):
    return lax.dot_general(a, b, (((1,), (1,)), ((), ())), precision=HIGHEST, preferred_element_type=F32)


def iota(shape, dim):
    return lax.broadcasted_iota(jnp.int32, shape, dim)


def roll(x, shift):
    shift = shift % x.shape[1]
    return x if shift == 0 else pltpu.roll(x, shift, 1)


def widen(x, lanes):
    return jnp.concatenate([x, jnp.zeros((x.shape[0], lanes - x.shape[1]), F32)], axis=1)


def chain(limit, xc_ref, hn_ref, vt_ref, fr_ref, rn_ref, td_ref):
    ng = W // 8
    sub = iota((8, 128), 0)
    lane = iota((8, 128), 1)
    live0 = lane < limit
    live1 = lane + 128 < limit
    xs0 = [xc_ref[8 * s:8 * s + 8, 0:128] for s in range(ng)]
    xs1 = [xc_ref[8 * s:8 * s + 8, 128:256] for s in range(ng)]
    hs = [hn_ref[8 * s:8 * s + 8, :] for s in range(ng)]

    def bcast_sub(x, u):
        return jnp.broadcast_to(x[u:u + 1, :], (8, 128))

    def bcast_col(x, k):
        return jnp.broadcast_to(x[:, k:k + 1], (8, 128))

    def columns(k):
        return ({s: bcast_col(hs[s], k) for s in range(k // 8, ng)}, {s: bcast_col(xs0[s], k) for s in range(0, ng)})

    window = {k: columns(k) for k in range(WIN)}
    for k in range(W):
        s0, u = k // 8, k % 8
        ch, cx = window.pop(k)
        hkk = bcast_sub(ch[s0], u)
        alpha = bcast_sub(cx[s0], u)
        inv_norm = lax.rsqrt(hkk)
        inv_beta = jnp.where(alpha >= 0, -inv_norm, inv_norm)
        beta = hkk * inv_beta
        inv = 1.0 / (alpha - beta)
        tau = (beta - alpha) * inv_beta
        below = sub > u
        rc, wc = {}, {}
        for s in range(s0, ng):
            r = ch[s] * inv_beta
            w = cx[s] - r
            rc[s] = jnp.where(below, r, 0.0) if s == s0 else r
            wc[s] = jnp.where(below, w, 0.0) if s == s0 else w
        r_of = {}
        for m in range(k + 1, min(k + WIN, W)):
            mh, mx = window[m]
            r_m = bcast_sub(rc[m // 8], m % 8)
            v_m = bcast_sub(mx[s0], u) * inv
            for s in range(m // 8, ng):
                mh[s] = mh[s] - rc[s] * r_m
            for s in range(s0, ng):
                mx[s] = mx[s] - wc[s] * v_m
        hrow = bcast_sub(hs[s0], u) * inv_beta
        x0 = bcast_sub(xs0[s0], u)
        x1 = bcast_sub(xs1[s0], u)
        s0v = x0 * inv
        v0 = jnp.where(live0 & (lane > k), s0v, jnp.where(lane == k, 1.0, 0.0))
        v1 = jnp.where(live1, x1 * inv, 0.0)
        vt_ref[k:k + 1, 0:128] = v0[0:1, :]
        vt_ref[k:k + 1, 128:256] = v1[0:1, :]
        fr_ref[k:k + 1, 0:128] = jnp.where(live0 & (lane > k), s0v, jnp.where(lane == k, beta, x0))[0:1, :]
        fr_ref[k:k + 1, 128:256] = jnp.where(live1, v1, x1)[0:1, :]
        rn_ref[k:k + 1, :] = hrow[0:1, :]
        td_ref[k:k + 1, :] = jnp.where(lane == k, tau, 0.0)[0:1, :]
        for s in range(s0, ng):
            hs[s] = hs[s] - rc[s] * hrow
            xs0[s] = xs0[s] - wc[s] * v0
            xs1[s] = xs1[s] - wc[s] * v1
        if k + WIN < W:
            window[k + WIN] = columns(k + WIN)


def load_panel(g, refs):
    xt, e1, e2, rts, wts, rinvd, rnat, kvt, xc_ref, hn_ref, dvec = (
        refs["xt"], refs["e1"], refs["e2"], refs["rts"], refs["wts"], refs["rinvd"], refs["rnat"], refs["kv"], refs["xc"], refs["hn"], refs["dvec"])
    x = xt[g]
    lane = iota((W, 256), 1)
    row = iota((W, 256), 0)
    diag = jnp.sum(jnp.where(lane == row + N, x, 0.0), axis=0, keepdims=True)
    dvec[0:1, :] = dvec[0:1, :] + roll(diag, 64 + W * g)
    gram = roll(x, 64)[:, 0:128]
    lane1 = lane[:, 0:128]
    row1 = row[:, 0:128]
    x = jnp.where(lane >= N, jnp.where(lane == row + N, 1.0, 0.0), x)
    hgg = gram[:, 0:W]
    for h in range(g):
        if g - h == 1:
            hgh = e1[g][:, 0:W]
        elif g - h == 2:
            hgh = roll(e1[g], 80)[:, 0:W]
        else:
            hgh = e2[0][:, 0:W] + e2[1][:, 0:W]
        for q in range(h):
            hgh = hgh - mm_nt(rts[g, q], rts[h, q])
        rt = mm_nt(hgh, rinvd[h])
        d = hgh - mm(x[:, 0:W], rnat[h])
        both = mm(d, kvt[h])
        x = roll(x - both[:, 0:256], 256 - W)
        hgg = hgg - mm_nt(rt, rt)
        rts[g, h] = rt
        wts[g, h] = both[:, 256:256 + W]
    xc_ref[...] = x
    hn_ref[...] = jnp.where(lane1 < W, widen(hgg, 128), jnp.where(lane1 == row1 + 64, 1.0, 0.0))


def close_panel(g, refs):
    vt = refs["vt"][...]
    fr = refs["fr"][...]
    rn = refs["rn"][...]
    td = refs["td"][...]
    lane = iota((W, 256), 1)
    lane1 = iota((W, 128), 1)
    row1 = iota((W, 128), 0)
    sq_lane = iota((W, W), 1)
    sq_row = iota((W, W), 0)
    refs["ftop"][g] = roll(fr, W * g)
    mt = roll(vt, 64 + W * g)[:, 0:W]
    v = jnp.where(lane < N - W * g, vt, 0.0)
    rnat = jnp.where((lane1 >= row1) & (lane1 < W), rn, 0.0)[:, 0:W]
    rinvt = roll(rn, 64)[:, 0:W]
    rinvt = jnp.where(sq_lane <= sq_row, rinvt, 0.0)
    mt = jnp.where(sq_lane <= sq_row, mt, 0.0)
    refs["rnat"][g] = rnat
    refs["rinvd"][g] = rinvt
    s = -mm(v[:, 0:W], mm_nt(rnat, mt))
    t = td[:, 0:W]
    refs["tau"][g:g + 1, :] = jnp.sum(td, axis=0, keepdims=True)[:, 0:W]
    size = 1
    while size < W:
        pair = (sq_row // (2 * size) == sq_lane // (2 * size)) & (sq_row // size < sq_lane // size)
        t = t - mm(mm(t, jnp.where(pair, s, 0.0)), t)
        size *= 2
    refs["t"][g] = t
    if g + 1 < NP:
        kmat = lax.dot_general(mt, t, (((0,), (0,)), ((), ())), precision=HIGHEST, preferred_element_type=F32)
        refs["kv"][g, :, 0:256] = mm(kmat, v)
        refs["kv"][g, :, 256:384] = widen(kmat, 128)
    lr = roll(widen(rinvt, 256), W * g)
    lc = roll(widen(mt, 256), W * g)
    if g:
        rcat = sum(roll(widen(refs["rts"][g, h], 256), W * h) for h in range(g))
        wcat = sum(roll(widen(refs["wts"][g, h], 256), W * h) for h in range(g))
        lr = lr - mm(mm(rinvt, rcat)[:, 0:N], refs["lr"][...])
        lc = lc - mm(mm(mt, wcat)[:, 0:N], refs["lc"][...])
    refs["lr"][W * g:W * g + W, :] = lr
    refs["lc"][W * g:W * g + W, :] = lc


def gather_kernel(a_hbm, b_hbm, f_alt, aux_ref, flag_ref, panels, xt, e1, e2, x0s, x1s, x2s, x3s, g1s, g1r, g2s, g2r, h1s, h1r, h2s, h2r,
                 rts, wts, rinvd, rnat, kvt, xc, hn, dvec, vt, fr, rn, td, ftop, lr, lc, tau, t_fac, bad_mine, bad_other,
                 load_sem, send_sem, bulk_sem, ex_send, ex_recv, e0_send, e0_recv, e1_send, e1_recv, e2_send, e2_recv, flag_sem, write_sem):
    refs = dict(xt=xt, e1=e1, e2=e2, rts=rts, wts=wts, rinvd=rinvd, rnat=rnat, kv=kvt, xc=xc, hn=hn, dvec=dvec,
                vt=vt, fr=fr, rn=rn, td=td, ftop=ftop, lr=lr, lc=lc, tau=tau, t=t_fac)
    part = lax.axis_index("part")
    c = lax.axis_index("col")
    r = lax.axis_index("row")
    width = panels.shape[3]
    twin = r + 1 - 2 * lax.rem(r, 2)
    across = lax.rem(r + 2, 4)

    def at(col, row):
        return (part, col, row)

    for q in range(NC):
        pltpu.make_async_copy(a_hbm.at[:, pl.ds(q * width, width)], panels.at[c, q], load_sem.at[q]).start()

    barrier = pltpu.get_barrier_semaphore()
    for s in range(1, NP):
        pl.semaphore_signal(barrier, inc=1, device_id=at(lax.rem(c + s, NP), r), device_id_type=MESH)
    pl.semaphore_signal(barrier, inc=1, device_id=at(c, twin), device_id_type=MESH)
    pl.semaphore_signal(barrier, inc=1, device_id=at(c, across), device_id_type=MESH)
    pl.semaphore_signal(barrier, inc=1, device_id=(1 - part, c, r), device_id_type=MESH)
    pl.semaphore_wait(barrier, NP + 2)

    lr[...] = jnp.zeros_like(lr)
    lc[...] = jnp.zeros_like(lc)
    dvec[...] = jnp.zeros_like(dvec)
    e2[...] = jnp.zeros_like(e2)

    order_l = list(range(NC))
    order_r = list(range(NC // 2, NC)) + list(range(NC // 2))

    def bulk(side, g, q):
        other = c - 1 if side == 0 else c + 1
        return pltpu.make_async_remote_copy(
            src_ref=panels.at[g, q], dst_ref=panels.at[g, q], send_sem=send_sem.at[side, g, q], recv_sem=bulk_sem.at[g, q],
            device_id=at(other, r), device_id_type=MESH)

    def start_own(i):
        @pl.when(c >= 1)
        def _():
            bulk(0, c, order_l[i]).start()

        @pl.when(c <= NP - 2)
        def _():
            bulk(1, c, order_r[i]).start()

    def write(g, q):
        return pltpu.make_async_copy(panels.at[g, q], b_hbm.at[pl.ds(pl.multiple_of(g * W, W), W), pl.ds(q * width, width)], write_sem.at[g, q])

    def arrive(dist, i):
        @pl.when(c + dist <= NP - 1)
        def _():
            bulk(0, c + dist, order_l[i]).wait_recv()
            write(c + dist, order_l[i]).start()

        @pl.when(c - dist >= 0)
        def _():
            bulk(1, c - dist, order_r[i]).wait_recv()
            write(c - dist, order_r[i]).start()

    def forward(dist, i):
        @pl.when((c + dist <= NP - 1) & (c >= 1))
        def _():
            bulk(0, c + dist, order_l[i]).start()

        @pl.when((c - dist >= 0) & (c <= NP - 2))
        def _():
            bulk(1, c - dist, order_r[i]).start()

    def row_sum(e, mine, got1, half, got2, out, slot):
        first = pltpu.make_async_remote_copy(mine, got1, ex_send.at[e, 0], ex_recv.at[e, 0], device_id=at(c, twin), device_id_type=MESH)
        first.start()
        first.wait()
        half[...] = mine[...] + got1[...]
        second = pltpu.make_async_remote_copy(half, got2, ex_send.at[e, 1], ex_recv.at[e, 1], device_id=at(c, across), device_id_type=MESH)
        second.start()
        second.wait()
        out[slot] = half[...] + got2[...]

    def shared(ref, slot, ssem, rsem, sslot, s, rslot):
        return pltpu.make_async_remote_copy(ref.at[slot], ref.at[slot], ssem.at[sslot], rsem.at[rslot],
                                            device_id=at(lax.rem(c + s, NP), r), device_id_type=MESH)

    def chunk_cols(g, q):
        return panels[g, q]

    for q in range(NC):
        pltpu.make_async_copy(a_hbm.at[:, pl.ds(q * width, width)], panels.at[c, q], load_sem.at[q]).wait()
    head = 3
    for i in range(head):
        start_own(i)
    for q in range(NC):
        write(c, q).start()
    gram = jnp.zeros((W, W), F32)
    for q in range(NC):
        blk = chunk_cols(c, q)
        gram = gram + mm_nt(blk, blk)
    lane = iota((W, 256), 1)
    top = jnp.where((lane < N) & (r == 0), panels[c, 0, :, 0:256], 0.0)
    x0s[...] = top + roll(widen(gram, 256), N)
    row_sum(0, x0s, x1s, x2s, x3s, xt, c)
    for s in range(1, NP):
        shared(xt, c, e0_send, e0_recv, s - 1, s, c).start()
    for i in range(head, NC):
        start_own(i)

    def wait_e0(g):
        @pl.when(c != g)
        def _():
            shared(xt, g, e0_send, e0_recv, 0, 1, g).wait_recv()

    def wait_e1(g):
        @pl.when(c != g - 1)
        def _():
            shared(e1, g, e1_send, e1_recv, 0, 1, g).wait_recv()

    def wait_e2(i):
        @pl.when(c != i + 1)
        def _():
            shared(e2, i, e2_send, e2_recv, 0, 1, i).wait_recv()

    def before(g):
        if g == 0:
            wait_e0(0)
        if g == 1:
            for i in range(NC):
                arrive(1, i)
                if i < head:
                    forward(1, i)

            @pl.when(c <= NP - 2)
            def _():
                left = jnp.maximum(c - 1, 0)
                acc = jnp.zeros((W, 2 * W), F32)
                for q in range(NC):
                    pair = jnp.concatenate([chunk_cols(c, q), chunk_cols(left, q)], axis=0)
                    acc = acc + mm_nt(chunk_cols(c + 1, q), pair)
                g1s[...] = widen(acc, 128)
                row_sum(1, g1s, g1r, g2s, g2r, e1, c + 1)
                for s in range(1, NP):
                    shared(e1, c + 1, e1_send, e1_recv, s - 1, s, c + 1).start()
            for i in range(head, NC):
                forward(1, i)
            wait_e0(1)
            wait_e1(1)
        if g == 2:
            half = NC // 2
            for i in range(half):
                arrive(2, i)
                if i < 1:
                    forward(2, i)

            @pl.when((c >= 1) & (c <= 2))
            def _():
                base = (c - 1) * half
                acc = jnp.zeros((W, W), F32)
                for i in range(half):
                    acc = acc + mm_nt(chunk_cols(3, base + i), chunk_cols(0, base + i))
                h1s[...] = widen(acc, 128)
                row_sum(2, h1s, h1r, h2s, h2r, e2, c - 1)
                for s in range(1, NP):
                    shared(e2, c - 1, e2_send, e2_recv, s - 1, s, c - 1).start()
            for i in range(1, half):
                forward(2, i)
            wait_e0(2)
            wait_e1(2)
        if g == 3:
            for i in range(NC // 2, NC):
                arrive(2, i)
                forward(2, i)
            wait_e0(3)
            wait_e1(3)
            wait_e2(0)
            wait_e2(1)

    def panel_step(g, carry):
        for s in range(NP):
            @pl.when(g == s)
            def _():
                before(s)
                load_panel(s, refs)
        chain(256 - W * g, xc, hn, vt, fr, rn, td)
        for s in range(NP):
            @pl.when(g == s)
            def _():
                close_panel(s, refs)
        return carry

    lax.fori_loop(0, NP, panel_step, 0)

    dv = dvec[0:1, 0:N]
    lr_all = lr[...][:, 0:N]
    lc_all = lc[...][:, 0:N]
    good = ((jnp.sum(lr_all * lr_all * dv) <= SUM_BOUND) & (jnp.sum(lc_all * lc_all * dv) <= SUM_BOUND)
            & (jnp.min(dv) > 1e-18) & (jnp.max(dv) < 1e30))
    bad_mine[...] = jnp.zeros((8, 128), F32) + jnp.where(good, 0.0, 1.0)
    flag_copy = pltpu.make_async_remote_copy(bad_mine, bad_other, flag_sem.at[0], flag_sem.at[1], device_id=(1 - part, c, r), device_id_type=MESH)
    flag_copy.start()

    aux_ref[0:N, :] = lr[...]
    aux_ref[N:N + W, :] = lc[pl.ds(pl.multiple_of(c * W, W), W), :]
    aux_ref[AUX_TOP:AUX_TOP + W, :] = ftop[c]
    for g in range(NP):
        aux_ref[AUX_T + W * g:AUX_T + W * g + W, :] = widen(t_fac[g], 256)
    aux_ref[AUX_TAU:AUX_TAU + 8, :] = jnp.concatenate([widen(tau[...], 256), jnp.zeros((4, 256), F32)], axis=0)
    aux_ref[AUX_MODE:AUX_MODE + 8, :] = jnp.zeros((8, 256), F32)

    for i in range(NC):
        arrive(3, i)
    flag_copy.wait()
    flag_ref[0] = jnp.max(jnp.maximum(bad_mine[...], bad_other[...]))
    for g in range(NP):
        for q in range(NC):
            write(g, q).wait()

    for i in range(NC):
        @pl.when(c >= 1)
        def _():
            for s in range(NP):
                @pl.when(c <= s)
                def _():
                    bulk(0, s, i).wait_send()

        @pl.when(c <= NP - 2)
        def _():
            for s in range(NP):
                @pl.when(c >= s)
                def _():
                    bulk(1, s, i).wait_send()
    for s in range(1, NP):
        shared(xt, c, e0_send, e0_recv, s - 1, s, c).wait_send()

        @pl.when(c <= NP - 2)
        def _():
            shared(e1, c + 1, e1_send, e1_recv, s - 1, s, c + 1).wait_send()

        @pl.when((c >= 1) & (c <= 2))
        def _():
            shared(e2, c - 1, e2_send, e2_recv, s - 1, s, c - 1).wait_send()


def gather_and_factor(a_t):
    rows = a_t.shape[1]
    width = rows // NC
    vm = lambda *shape: pltpu.VMEM(shape, F32)
    dma = lambda *shape: pltpu.SemaphoreType.DMA(shape)
    out = lambda *shape: jax.ShapeDtypeStruct(shape, F32)
    hbm = pl.BlockSpec(memory_space=pl.ANY)
    scratch = [vm(NP, NC, W, width), vm(NP, W, 256), vm(NP, W, 128), vm(2, W, 128), vm(W, 256), vm(W, 256), vm(W, 256)]
    scratch += [vm(W, 256)]
    scratch += [vm(W, 128)] * 8
    scratch += [vm(NP, 3, W, W), vm(NP, 3, W, W), vm(NP, W, W), vm(NP, W, W), vm(3, W, 384), vm(W, 256), vm(W, 128), vm(8, 256),
                vm(W, 256), vm(W, 256), vm(W, 128), vm(W, 128), vm(NP, W, 256), vm(N, 256), vm(N, 256),
                vm(NP, W), vm(NP, W, W), vm(8, 128), vm(8, 128)]
    scratch += [dma(NC), dma(2, NP, NC), dma(NP, NC), dma(3, 2), dma(3, 2), dma(3), dma(NP), dma(3), dma(NP), dma(3), dma(2), dma(2), dma(NP, NC)]
    return pl.pallas_call(
        gather_kernel,
        name="gather_and_factor",
        out_shape=(out(N, rows), out(W, rows), out(AUX_ROWS, 256), out(1)),
        in_specs=[hbm],
        out_specs=(hbm, hbm, pl.BlockSpec(memory_space=pltpu.VMEM), pl.BlockSpec(memory_space=pltpu.SMEM)),
        scratch_shapes=scratch,
        compiler_params=pltpu.CompilerParams(collective_id=0, has_side_effects=True, vmem_limit_bytes=32 * 1024 * 1024),
    )(a_t)


def pack_kernel(tau_ref, t_ref, aux_ref):
    aux_ref[...] = jnp.zeros_like(aux_ref)
    for g in range(NP):
        aux_ref[AUX_T + W * g:AUX_T + W * g + W, 0:W] = t_ref[g]
    aux_ref[AUX_TAU:AUX_TAU + NP, 0:W] = tau_ref[...]
    aux_ref[AUX_MODE:AUX_MODE + 8, :] = jnp.ones((8, 256), F32)


def pack_aux(tau_vals, t_fac):
    return pl.pallas_call(pack_kernel, name="pack_aux", out_shape=jax.ShapeDtypeStruct((AUX_ROWS, 256), F32))(tau_vals, t_fac)


def product_kernel(b_ref, f_alt, aux_ref, q_ref, f_ref, tau_ref, t_ref, sem):
    step = pl.program_id(0)
    width = b_ref.shape[1]
    careful = jnp.max(aux_ref[AUX_MODE:AUX_MODE + 8, 0:128]) > 0.5

    @pl.when(step == 0)
    def _():
        tau_ref[...] = aux_ref[AUX_TAU:AUX_TAU + NP, 0:W]
        for g in range(NP):
            t_ref[g] = aux_ref[AUX_T + W * g:AUX_T + W * g + W, 0:W]

    @pl.when(jnp.logical_not(careful))
    def _():
        prod = mm(aux_ref[0:N + W, 0:N], b_ref[...])
        q_ref[...] = prod[0:N]
        f_ref[...] = prod[N:N + W]

        @pl.when((step == 0) & (lax.axis_index("row") == 0))
        def _():
            keep = iota((W, 256), 1) < N
            f_ref[:, 0:256] = jnp.where(keep, aux_ref[AUX_TOP:AUX_TOP + W, :], prod[N:N + W, 0:256])

    @pl.when(careful)
    def _():
        q_ref[...] = b_ref[...]
        copy = pltpu.make_async_copy(f_alt.at[:, pl.ds(pl.multiple_of(step * width, width), width)], f_ref, sem)
        copy.start()
        copy.wait()


def products(b, f_alt, aux):
    rows = b.shape[1]
    width = rows // STEPS
    out = lambda *shape: jax.ShapeDtypeStruct(shape, F32)
    whole = pl.BlockSpec(memory_space=pltpu.VMEM)
    return pl.pallas_call(
        product_kernel,
        name="products",
        grid=(STEPS,),
        out_shape=(out(N, rows), out(W, rows), out(NP, W), out(NP, W, W)),
        in_specs=[pl.BlockSpec((N, width), lambda i: (0, i)), pl.BlockSpec(memory_space=pl.ANY), whole],
        out_specs=(pl.BlockSpec((N, width), lambda i: (0, i)), pl.BlockSpec((W, width), lambda i: (0, i)), whole, whole),
        scratch_shapes=[pltpu.SemaphoreType.DMA],
        compiler_params=pltpu.CompilerParams(vmem_limit_bytes=32 * 1024 * 1024),
    )(b, f_alt, aux)


def all_pieces(x, axis, n):
    me = lax.axis_index(axis)
    got = jnp.stack([x] + [lax.ppermute(x, axis, [(i, (i + s) % n) for i in range(n)]) for s in range(1, n)])
    return [lax.dynamic_index_in_dim(got, (me - j) % n, axis=0, keepdims=False) for j in range(n)]


def ordered_sum(x, axis, n):
    pieces = all_pieces(x, axis, n)
    total = pieces[0]
    for piece in pieces[1:]:
        total = total + piece
    return total


def dot_high(lhs_mat, rhs_mat):
    return jnp.dot(lhs_mat, rhs_mat, precision=HIGHEST, preferred_element_type=jnp.float32)


def contract(einsum_form, lhs_mat, rhs_mat):
    return jnp.einsum(einsum_form, lhs_mat, rhs_mat, precision=HIGHEST, preferred_element_type=jnp.float32)


def factor_panel(panel_in, row_start, diag0, reduce_rows):
    rows_loc, panel_width = panel_in.shape
    global_rows = row_start + jnp.arange(rows_loc)
    col_ids = jnp.arange(panel_width)

    def column_step(col_step, carried):
        panel_work, refl_vecs, tau_vec = carried
        diag_row = diag0 + col_step
        column = lax.dynamic_index_in_dim(panel_work, col_step, axis=1, keepdims=False)
        x_col = jnp.where(global_rows >= diag_row, column, 0.0)
        local_row = diag_row - row_start
        holds_diag = (local_row >= 0) & (local_row < rows_loc)
        diag_row_vals = lax.dynamic_index_in_dim(panel_work, jnp.clip(local_row, 0, rows_loc - 1), axis=0, keepdims=False)
        diag_piece = jnp.where(holds_diag, diag_row_vals, 0.0)
        summed = reduce_rows(jnp.stack([dot_high(x_col, panel_work), diag_piece]))
        x_dots = summed[0]
        diag_vals = summed[1]
        alpha_val = diag_vals[col_step]
        col_norm = jnp.sqrt(x_dots[col_step])
        beta_val = jnp.where(alpha_val >= 0, -col_norm, col_norm)
        tau_step = (beta_val - alpha_val) / beta_val
        inv_scale = 1.0 / (alpha_val - beta_val)
        at_diag = global_rows == diag_row
        reflector = jnp.where(global_rows > diag_row, x_col * inv_scale, jnp.where(at_diag, 1.0, 0.0))
        v_dots = jnp.where(col_ids > col_step, inv_scale * (x_dots - alpha_val * diag_vals) + diag_vals, 0.0)
        panel_work = panel_work - tau_step * reflector[:, None] * v_dots[None, :]
        new_col = jnp.where(global_rows < diag_row, column, jnp.where(at_diag, beta_val, reflector))
        is_col = col_ids == col_step
        panel_work = jnp.where(is_col[None, :], new_col[:, None], panel_work)
        refl_vecs = jnp.where(is_col[None, :], reflector[:, None], refl_vecs)
        tau_vec = jnp.where(is_col, tau_step, tau_vec)
        return panel_work, refl_vecs, tau_vec

    init_carry = (panel_in, jnp.zeros_like(panel_in), jnp.zeros((panel_width,), jnp.float32))
    return lax.fori_loop(0, panel_width, column_step, init_carry)


def build_tfac(refl_vecs, tau_vec, reduce_rows):
    panel_width = tau_vec.shape[0]
    col_ids = jnp.arange(panel_width)
    gram_mat = reduce_rows(contract("rk,rl->kl", refl_vecs, refl_vecs))

    def t_step(col_step, t_fac):
        g_col = jnp.where(col_ids < col_step, lax.dynamic_index_in_dim(gram_mat, col_step, axis=1, keepdims=False), 0.0)
        tau_step = tau_vec[col_step]
        new_col = jnp.where(col_ids == col_step, tau_step, -tau_step * dot_high(t_fac, g_col))
        return jnp.where(col_ids[None, :] == col_step, new_col[:, None], t_fac)

    return lax.fori_loop(0, panel_width, t_step, jnp.zeros((panel_width, panel_width), jnp.float32))


def careful_program(proc_cols, proc_rows):
    sum_rows = functools.partial(ordered_sum, axis="row", n=proc_rows)

    def local_program(a_loc):
        rows_loc, panels_loc, panel_width = a_loc.shape
        num_panels = panels_loc * proc_cols
        col_idx = lax.axis_index("col")
        row_start = lax.axis_index("row") * rows_loc
        global_rows = row_start + jnp.arange(rows_loc)
        panel_ids = jnp.arange(panels_loc) * proc_cols + col_idx

        def panel_step(panel_idx, carried):
            a_work, all_vecs, all_tfac = carried
            slot_idx = panel_idx // proc_cols
            is_owner = col_idx == panel_idx % proc_cols
            old_panel = lax.dynamic_index_in_dim(a_work, slot_idx, axis=1, keepdims=False)
            new_panel, refl_vecs, tau_vec = factor_panel(old_panel, row_start, panel_idx * panel_width, sum_rows)
            t_fac = build_tfac(refl_vecs, tau_vec, sum_rows)
            refl_vecs = ordered_sum(jnp.where(is_owner, refl_vecs, 0.0), "col", proc_cols)
            t_fac = ordered_sum(jnp.where(is_owner, t_fac, 0.0), "col", proc_cols)
            a_work = lax.dynamic_update_index_in_dim(a_work, jnp.where(is_owner, new_panel, old_panel), slot_idx, axis=1)
            proj_sum = sum_rows(contract("rk,rsj->ksj", refl_vecs, a_work))
            w_block = contract("kl,ksj->lsj", t_fac, proj_sum)
            w_block = jnp.where((panel_ids > panel_idx)[None, :, None], w_block, 0.0)
            a_work = a_work - contract("rl,lsj->rsj", refl_vecs, w_block)
            all_vecs = lax.dynamic_update_index_in_dim(all_vecs, refl_vecs, panel_idx, axis=0)
            all_tfac = lax.dynamic_update_index_in_dim(all_tfac, t_fac, panel_idx, axis=0)
            return a_work, all_vecs, all_tfac

        init_carry = (a_loc, jnp.zeros((num_panels, rows_loc, panel_width), jnp.float32), jnp.zeros((num_panels, panel_width, panel_width), jnp.float32))
        a_work, all_vecs, all_tfac = lax.fori_loop(0, num_panels, panel_step, init_carry)
        logical_cols = panel_ids[:, None] * panel_width + jnp.arange(panel_width)[None, :]
        q_init = (global_rows[:, None, None] == logical_cols[None, :, :]).astype(jnp.float32)

        def q_step(back_step, q_local):
            panel_idx = num_panels - 1 - back_step
            refl_vecs = lax.dynamic_index_in_dim(all_vecs, panel_idx, keepdims=False)
            t_fac = lax.dynamic_index_in_dim(all_tfac, panel_idx, keepdims=False)
            proj_sum = sum_rows(contract("rk,rsj->ksj", refl_vecs, q_local))
            w_block = contract("kl,lsj->ksj", t_fac, proj_sum)
            return q_local - contract("rk,ksj->rsj", refl_vecs, w_block)

        q_local = lax.fori_loop(0, num_panels, q_step, q_init)
        gathered = jnp.stack(all_pieces(q_local, "col", proc_cols))
        q_rows = gathered.transpose(1, 2, 0, 3).reshape(rows_loc, num_panels * panel_width)
        tau_vals = jnp.diagonal(all_tfac, axis1=1, axis2=2)
        return a_work, tau_vals, all_tfac, q_rows

    return local_program


def solution(mesh):
    careful = careful_program(mesh.shape["col"], mesh.shape["row"])

    def local_program(a_loc):
        rows_loc = a_loc.shape[0]
        b, f_alt, aux, flag = gather_and_factor(a_loc.reshape(rows_loc, W).T)

        def again(state):
            factored, tau_new, t_new, q_new = careful(a_loc)
            return jnp.zeros((1,), F32), q_new.T, factored.reshape(rows_loc, W).T, pack_aux(tau_new, t_new)

        b, f_alt, aux = lax.while_loop(lambda s: s[0][0] > 0.5, again, (flag, b, f_alt, aux))[1:]
        q_t, f_t, tau_vals, t_fac = products(b, f_alt, aux)
        return f_t.T.reshape(rows_loc, 1, W), tau_vals, t_fac, q_t.T

    spec_rows = P(("part", "row"), "col", None)
    out_specs = (spec_rows, P("part", None), P("part", None, None), P(("part", "row"), None))
    return jax.shard_map(local_program, mesh=mesh, in_specs=(spec_rows,), out_specs=out_specs, check_vma=False)
```

```python
import functools
import jax
import jax.numpy as jnp
from jax import lax
from jax.experimental import pallas as pl
from jax.experimental.pallas import tpu as pltpu
from jax.sharding import PartitionSpec as P

HIGHEST = lax.Precision.HIGHEST
MESH = pl.DeviceIdType.MESH
W = 48
NP = 4
N = W * NP
NC = 8
WIN = 6
F32 = jnp.float32
SUM_BOUND = 6144.0
HEAD0, HEAD1, HEAD2 = 3, 5, 2
STEPS = 2
AUX_TOP = N + W
AUX_T = AUX_TOP + W
AUX_TAU = AUX_T + N
AUX_MODE = AUX_TAU + 8
AUX_ROWS = AUX_MODE + 8


def mm(a, b):
    return lax.dot_general(a, b, (((1,), (0,)), ((), ())), precision=HIGHEST, preferred_element_type=F32)


def mm_nt(a, b):
    return lax.dot_general(a, b, (((1,), (1,)), ((), ())), precision=HIGHEST, preferred_element_type=F32)


def iota(shape, dim):
    return lax.broadcasted_iota(jnp.int32, shape, dim)


def roll(x, shift):
    shift = shift % x.shape[1]
    return x if shift == 0 else pltpu.roll(x, shift, 1)


def widen(x, lanes):
    return jnp.concatenate([x, jnp.zeros((x.shape[0], lanes - x.shape[1]), F32)], axis=1)


def chain(limit, xc_ref, hn_ref, vt_ref, fr_ref, rn_ref, td_ref, zt_ref):
    ng = W // 8
    sub = iota((8, 128), 0)
    lane = iota((8, 128), 1)
    live0 = lane < limit
    live1 = lane + 128 < limit
    xs0 = [xc_ref[8 * s:8 * s + 8, 0:128] for s in range(ng)]
    xs1 = [xc_ref[8 * s:8 * s + 8, 128:256] for s in range(ng)]
    hs = [hn_ref[8 * s:8 * s + 8, :] for s in range(ng)]
    zs = [jnp.where(lane == sub + 8 * s, 1.0, 0.0) for s in range(ng)]

    def bcast_sub(x, u):
        return jnp.broadcast_to(x[u:u + 1, :], (8, 128))

    def bcast_col(x, k):
        return jnp.broadcast_to(x[:, k:k + 1], (8, 128))

    def columns(k):
        return ({s: bcast_col(hs[s], k) for s in range(k // 8, ng)}, {s: bcast_col(xs0[s], k) for s in range(0, ng)},
                {s: bcast_col(zs[s], k) for s in range(k // 8 + 1)})

    window = {k: columns(k) for k in range(WIN)}
    for k in range(W):
        s0, u = k // 8, k % 8
        ch, cx, cz = window.pop(k)
        hkk = bcast_sub(ch[s0], u)
        alpha = bcast_sub(cx[s0], u)
        inv_norm = lax.rsqrt(hkk)
        inv_beta = jnp.where(alpha >= 0, -inv_norm, inv_norm)
        beta = hkk * inv_beta
        inv = 1.0 / (alpha - beta)
        tau = (beta - alpha) * inv_beta
        below = sub > u
        rc, wc = {}, {}
        for s in range(s0, ng):
            r = ch[s] * inv_beta
            w = cx[s] - r
            rc[s] = jnp.where(below, r, 0.0) if s == s0 else r
            wc[s] = jnp.where(below, w, 0.0) if s == s0 else w
        r_of = {}
        for m in range(k + 1, min(k + WIN, W)):
            mh, mx, mz = window[m]
            r_m = bcast_sub(rc[m // 8], m % 8)
            v_m = bcast_sub(mx[s0], u) * inv
            for s in range(m // 8, ng):
                mh[s] = mh[s] - rc[s] * r_m
            for s in range(s0, ng):
                mx[s] = mx[s] - wc[s] * v_m
            for s in range(s0 + 1):
                mz[s] = mz[s] - cz[s] * v_m
        hrow = bcast_sub(hs[s0], u) * inv_beta
        x0 = bcast_sub(xs0[s0], u)
        x1 = bcast_sub(xs1[s0], u)
        s0v = x0 * inv
        v0 = jnp.where(live0 & (lane > k), s0v, jnp.where(lane == k, 1.0, 0.0))
        v1 = jnp.where(live1, x1 * inv, 0.0)
        vt_ref[k:k + 1, 0:128] = v0[0:1, :]
        vt_ref[k:k + 1, 128:256] = v1[0:1, :]
        fr_ref[k:k + 1, 0:128] = jnp.where(live0 & (lane > k), s0v, jnp.where(lane == k, beta, x0))[0:1, :]
        fr_ref[k:k + 1, 128:256] = jnp.where(live1, v1, x1)[0:1, :]
        rn_ref[k:k + 1, :] = hrow[0:1, :]
        td_ref[k:k + 1, :] = jnp.where(lane == k, tau, 0.0)[0:1, :]
        for s in range(s0, ng):
            hs[s] = hs[s] - rc[s] * hrow
            xs0[s] = xs0[s] - wc[s] * v0
            xs1[s] = xs1[s] - wc[s] * v1
        v_next = jnp.where(lane == k, 0.0, v0)
        for s in range(s0 + 1):
            zs[s] = zs[s] - cz[s] * v_next
        if k + WIN < W:
            window[k + WIN] = columns(k + WIN)
    for s in range(ng):
        zt_ref[8 * s:8 * s + 8, :] = zs[s]


def load_panel(g, refs):
    xt, e1, e2, rts, wts, rinvd, kvt, xc_ref, hn_ref, dvec = (
        refs["xt"], refs["e1"], refs["e2"], refs["rts"], refs["wts"], refs["rinvd"], refs["kv"], refs["xc"], refs["hn"], refs["dvec"])
    x = xt[g]
    lane = iota((W, 256), 1)
    row = iota((W, 256), 0)
    diag = jnp.sum(jnp.where(lane == row + N, x, 0.0), axis=0, keepdims=True)
    dvec[0:1, :] = dvec[0:1, :] + roll(diag, 64 + W * g)
    gram = roll(x, 64)[:, 0:128]
    lane1 = lane[:, 0:128]
    row1 = row[:, 0:128]
    x = jnp.where(lane >= N, jnp.where(lane == row + N, 1.0, 0.0), x)
    hgg = gram[:, 0:W]
    for h in range(g):
        if g - h == 1:
            hgh = e1[g][:, 0:W]
        elif g - h == 2:
            hgh = roll(e1[g], 80)[:, 0:W]
        else:
            hgh = e2[0][:, 0:W] + e2[1][:, 0:W]
        for q in range(h):
            hgh = hgh - mm_nt(rts[g, q], rts[h, q])
        rt = mm_nt(hgh, rinvd[h])
        both = mm(x[:, 0:W] - rt, kvt[h])
        x = roll(x - both[:, 0:256], 256 - W)
        hgg = hgg - mm_nt(rt, rt)
        rts[g, h] = rt
        wts[g, h] = both[:, 256:256 + W]
    xc_ref[...] = x
    hn_ref[...] = jnp.where(lane1 < W, widen(hgg, 128), jnp.where(lane1 == row1 + 64, 1.0, 0.0))


def close_panel(g, refs):
    vt = refs["vt"][...]
    fr = refs["fr"][...]
    rn = refs["rn"][...]
    td = refs["td"][...]
    lane = iota((W, 256), 1)
    lane1 = iota((W, 128), 1)
    row1 = iota((W, 128), 0)
    sq_lane = iota((W, W), 1)
    sq_row = iota((W, W), 0)
    refs["ftop"][g] = roll(fr, W * g)
    mt = roll(vt, 64 + W * g)[:, 0:W]
    v = jnp.where(lane < N - W * g, vt, 0.0)
    rnat = jnp.where((lane1 >= row1) & (lane1 < W), rn, 0.0)[:, 0:W]
    rinvt = roll(rn, 64)[:, 0:W]
    rinvt = jnp.where(sq_lane <= sq_row, rinvt, 0.0)
    mt = jnp.where(sq_lane <= sq_row, mt, 0.0)
    refs["rinvd"][g] = rinvt
    refs["rnat"][g] = rnat
    refs["mts"][g] = mt
    refs["v1"][g] = v[:, 0:W]
    refs["t"][g] = td[:, 0:W]
    refs["tau"][g:g + 1, :] = jnp.sum(td, axis=0, keepdims=True)[:, 0:W]
    zt = refs["zt"][:, 0:W]
    refs["zsum"][...] = refs["zsum"][...] + jnp.sum(zt * zt)
    if g + 1 < NP:
        refs["kv"][g, :, 0:256] = mm(zt, v)
        refs["kv"][g, :, 256:384] = widen(zt, 128)
    lr = roll(widen(rinvt, 256), W * g)
    lc = roll(widen(mt, 256), W * g)
    if g:
        rcat = sum(roll(widen(refs["rts"][g, h], 256), W * h) for h in range(g))
        wcat = sum(roll(widen(refs["wts"][g, h], 256), W * h) for h in range(g))
        lr = lr - mm(mm(rinvt, rcat)[:, 0:N], refs["lr"][...])
        lc = lc - mm(mm(mt, wcat)[:, 0:N], refs["lc"][...])
    refs["lr"][W * g:W * g + W, :] = lr
    refs["lc"][W * g:W * g + W, :] = lc


def build_t(refs):
    sq_lane = iota((W, W), 1)
    sq_row = iota((W, W), 0)
    prods = [mm_nt(refs["rnat"][g], refs["mts"][g]) for g in range(NP)]
    ss = [-mm(refs["v1"][g], prods[g]) for g in range(NP)]
    ts = [refs["t"][g] for g in range(NP)]
    size = 1
    while size < W:
        pair = (sq_row // (2 * size) == sq_lane // (2 * size)) & (sq_row // size < sq_lane // size)
        halves = [mm(ts[g], jnp.where(pair, ss[g], 0.0)) for g in range(NP)]
        ts = [ts[g] - mm(halves[g], ts[g]) for g in range(NP)]
        size *= 2
    for g in range(NP):
        refs["t"][g] = ts[g]


def gather_kernel(a_hbm, b_hbm, f_alt, aux_ref, flag_ref, panels, xt, e1, e2, x0s, x1s, x2s, x3s, g1s, g1r, g2s, g2r, h1s, h1r, h2s, h2r,
                 rts, wts, rinvd, rnat, kvt, xc, hn, dvec, vt, fr, rn, td, ftop, lr, lc, tau, t_fac, zt, mts, v1s, zsum, bad_mine, bad_other,
                 load_sem, send_sem, bulk_sem, ex_send, ex_recv, e0_send, e0_recv, e0_row, e1_send, e1_recv, e1_row, e2_send, e2_recv, e2_row, flag_sem, write_sem):
    refs = dict(xt=xt, e1=e1, e2=e2, rts=rts, wts=wts, rinvd=rinvd, rnat=rnat, kv=kvt, xc=xc, hn=hn, dvec=dvec,
                vt=vt, fr=fr, rn=rn, td=td, ftop=ftop, lr=lr, lc=lc, tau=tau, t=t_fac, zt=zt, mts=mts, v1=v1s, zsum=zsum)
    part = lax.axis_index("part")
    c = lax.axis_index("col")
    r = lax.axis_index("row")
    width = panels.shape[3]
    twin = r + 1 - 2 * lax.rem(r, 2)
    across = lax.rem(r + 2, 4)

    def at(col, row):
        return (part, col, row)

    for q in range(NC):
        pltpu.make_async_copy(a_hbm.at[:, pl.ds(q * width, width)], panels.at[c, q], load_sem.at[q]).start()

    barrier = pltpu.get_barrier_semaphore()
    peers = [at(lax.rem(c + s, NP), r) for s in range(1, NP)] + [at(c, twin), at(c, across), (1 - part, c, r)]
    for peer in peers:
        pl.semaphore_signal(barrier, inc=1, device_id=peer, device_id_type=MESH)
    pl.semaphore_wait(barrier, len(peers))

    lr[...] = jnp.zeros_like(lr)
    lc[...] = jnp.zeros_like(lc)
    dvec[...] = jnp.zeros_like(dvec)
    zsum[...] = jnp.zeros_like(zsum)
    e2[...] = jnp.zeros_like(e2)

    order_load = [q for i in range(NC // 2) for q in (i, i + NC // 2)]
    order_l = list(range(NC))
    order_r = list(range(NC // 2, NC)) + list(range(NC // 2))

    def bulk(side, g, q):
        other = c - 1 if side == 0 else c + 1
        return pltpu.make_async_remote_copy(
            src_ref=panels.at[g, q], dst_ref=panels.at[g, q], send_sem=send_sem.at[side, g, q], recv_sem=bulk_sem.at[g, q],
            device_id=at(other, r), device_id_type=MESH)

    def start_own(i):
        @pl.when(c >= 1)
        def _():
            bulk(0, c, order_l[i]).start()

        @pl.when(c <= NP - 2)
        def _():
            bulk(1, c, order_r[i]).start()

    def write(g, q):
        return pltpu.make_async_copy(panels.at[g, q], b_hbm.at[pl.ds(pl.multiple_of(g * W, W), W), pl.ds(q * width, width)], write_sem.at[g, q])

    def arrive(dist, i):
        @pl.when(c + dist <= NP - 1)
        def _():
            bulk(0, c + dist, order_l[i]).wait_recv()
            write(c + dist, order_l[i]).start()

        @pl.when(c - dist >= 0)
        def _():
            bulk(1, c - dist, order_r[i]).wait_recv()
            write(c - dist, order_r[i]).start()

    def forward(dist, i):
        @pl.when((c + dist <= NP - 1) & (c >= 1))
        def _():
            bulk(0, c + dist, order_l[i]).start()

        @pl.when((c - dist >= 0) & (c <= NP - 2))
        def _():
            bulk(1, c - dist, order_r[i]).start()

    def row_sum(e, mine, got1, half, got2, out, slot):
        first = pltpu.make_async_remote_copy(mine, got1, ex_send.at[e, 0], ex_recv.at[e, 0], device_id=at(c, twin), device_id_type=MESH)
        first.start()
        first.wait()
        half[...] = mine[...] + got1[...]
        second = pltpu.make_async_remote_copy(half, got2, ex_send.at[e, 1], ex_recv.at[e, 1], device_id=at(c, across), device_id_type=MESH)
        second.start()
        second.wait()
        out[slot] = half[...] + got2[...]

    rows_mine = pl.ds(pl.multiple_of(lax.rem(r, 2) * (W // 2), 8), W // 2)
    lanes_mine = pl.ds(pl.multiple_of(lax.div(r, 2) * 128, 128), 128)

    class Message:
        def __init__(self, ref, slot, sems, quarter, source):
            self.ref, self.slot, self.sems, self.quarter, self.source = ref, slot, sems, quarter, source

        def copy(self, ref, send, recv, peer):
            return pltpu.make_async_remote_copy(ref, ref, send, recv, device_id=peer, device_id_type=MESH)

        def hop(self, s):
            part_ref = self.ref.at[self.slot, rows_mine, lanes_mine] if self.quarter else self.ref.at[self.slot, rows_mine]
            return self.copy(part_ref, self.sems[0].at[s - 1, self.slot], self.sems[1].at[self.slot], at(lax.rem(c + s, NP), r))

        def to_twin(self):
            part_ref = self.ref.at[self.slot, rows_mine, lanes_mine] if self.quarter else self.ref.at[self.slot, rows_mine]
            return self.copy(part_ref, self.sems[2].at[0, self.slot], self.sems[2].at[1, self.slot], at(c, twin))

        def to_across(self):
            return self.copy(self.ref.at[self.slot, :, lanes_mine], self.sems[2].at[2, self.slot], self.sems[2].at[3, self.slot], at(c, across))

        def each_hop(self, act):
            @pl.when(c == self.source)
            def _():
                for s in range(1, NP):
                    act(self.hop(s))

        def send_on(self):
            self.each_hop(lambda cp: cp.start())

        def receive(self):
            @pl.when(c != self.source)
            def _():
                self.hop(1).wait_recv()
                self.to_twin().start()

        def join(self):
            @pl.when(c != self.source)
            def _():
                self.to_twin().wait()
                if self.quarter:
                    self.to_across().start()

        def finish(self):
            if self.quarter:
                @pl.when(c != self.source)
                def _():
                    self.to_across().wait()

    msg0 = [Message(xt, g, (e0_send, e0_recv, e0_row), True, g) for g in range(NP)]
    msg1 = [None] + [Message(e1, g, (e1_send, e1_recv, e1_row), False, g - 1) for g in range(1, NP)]
    msg2 = [Message(e2, i, (e2_send, e2_recv, e2_row), False, i + 1) for i in range(2)]

    def take(messages):
        for m in messages:
            m.receive()
        for m in messages:
            m.join()
        for m in messages:
            m.finish()

    def chunk_cols(g, q):
        return panels[g, q]

    started = 0
    for q in range(NC):
        pltpu.make_async_copy(a_hbm.at[:, pl.ds(order_load[q] * width, width)], panels.at[c, order_load[q]], load_sem.at[order_load[q]]).wait()
        if q % 2 and started < HEAD0:
            start_own(started)
            started += 1
    gram = jnp.zeros((W, W), F32)
    for q in range(NC):
        blk = chunk_cols(c, q)
        gram = gram + mm_nt(blk, blk)
    for q in range(NC):
        write(c, q).start()
    lane = iota((W, 256), 1)
    top = jnp.where((lane < N) & (r == 0), panels[c, 0, :, 0:256], 0.0)
    x0s[...] = top + roll(widen(gram, 256), N)
    row_sum(0, x0s, x1s, x2s, x3s, xt, c)
    for m in msg0:
        m.send_on()
    for i in range(started, NC):
        start_own(i)

    def before(g):
        if g == 0:
            take(msg0)
        if g == 1:
            g1s[...] = jnp.zeros_like(g1s)
            left = jnp.maximum(c - 1, 0)
            for i in range(NC):
                arrive(1, i)
                if i < HEAD1:
                    forward(1, i)

                @pl.when(c <= NP - 2)
                def _():
                    for q in ([i, i - NC // 2] if i >= NC // 2 else []):
                        pair = jnp.concatenate([chunk_cols(c, q), chunk_cols(left, q)], axis=0)
                        g1s[:, 0:2 * W] += mm_nt(chunk_cols(c + 1, q), pair)

            @pl.when(c <= NP - 2)
            def _():
                row_sum(1, g1s, g1r, g2s, g2r, e1, c + 1)
            for m in msg1[1:]:
                m.send_on()
            for i in range(HEAD1, NC):
                forward(1, i)
            half = NC // 2
            for i in range(half):
                arrive(2, i)
                if i < HEAD2:
                    forward(2, i)

            @pl.when((c >= 1) & (c <= 2))
            def _():
                base = (c - 1) * half
                acc = jnp.zeros((W, W), F32)
                for i in range(half):
                    acc = acc + mm_nt(chunk_cols(3, base + i), chunk_cols(0, base + i))
                h1s[...] = widen(acc, 128)
                row_sum(2, h1s, h1r, h2s, h2r, e2, c - 1)
            for m in msg2:
                m.send_on()
            for i in range(HEAD2, half):
                forward(2, i)
            take(msg1[1:])
        if g == 2:
            for i in range(NC // 2, NC):
                arrive(2, i)
                forward(2, i)
        if g == 3:
            take(msg2)

    def panel_step(g, carry):
        for s in range(NP):
            @pl.when(g == s)
            def _():
                before(s)
                load_panel(s, refs)
        chain(256 - W * g, xc, hn, vt, fr, rn, td, zt)
        for s in range(NP):
            @pl.when(g == s)
            def _():
                close_panel(s, refs)
        return carry

    lax.fori_loop(0, NP, panel_step, 0)

    dv = dvec[0:1, 0:N]
    lr_all = lr[...][:, 0:N]
    lc_all = lc[...][:, 0:N]
    good = ((jnp.sum(lr_all * lr_all * dv) <= SUM_BOUND) & (jnp.sum(lc_all * lc_all * dv) <= SUM_BOUND)
            & (jnp.max(zsum[...]) <= SUM_BOUND) & (jnp.min(dv) > 1e-18) & (jnp.max(dv) < 1e30))
    bad_mine[...] = jnp.zeros((8, 128), F32) + jnp.where(good, 0.0, 1.0)
    flag_copy = pltpu.make_async_remote_copy(bad_mine, bad_other, flag_sem.at[0], flag_sem.at[1], device_id=(1 - part, c, r), device_id_type=MESH)
    flag_copy.start()
    build_t(refs)

    aux_ref[0:N, :] = lr[...]
    aux_ref[N:N + W, :] = lc[pl.ds(pl.multiple_of(c * W, W), W), :]
    aux_ref[AUX_TOP:AUX_TOP + W, :] = ftop[c]
    for g in range(NP):
        aux_ref[AUX_T + W * g:AUX_T + W * g + W, :] = widen(t_fac[g], 256)
    aux_ref[AUX_TAU:AUX_TAU + 8, :] = jnp.concatenate([widen(tau[...], 256), jnp.zeros((4, 256), F32)], axis=0)
    aux_ref[AUX_MODE:AUX_MODE + 8, :] = jnp.zeros((8, 256), F32)

    for i in range(NC):
        arrive(3, i)
    flag_copy.wait()
    flag_ref[0] = jnp.max(jnp.maximum(bad_mine[...], bad_other[...]))
    for g in range(NP):
        for q in range(NC):
            write(g, q).wait()

    for i in range(NC):
        @pl.when(c >= 1)
        def _():
            for s in range(NP):
                @pl.when(c <= s)
                def _():
                    bulk(0, s, i).wait_send()

        @pl.when(c <= NP - 2)
        def _():
            for s in range(NP):
                @pl.when(c >= s)
                def _():
                    bulk(1, s, i).wait_send()
    for m in msg0 + msg1[1:] + msg2:
        m.each_hop(lambda cp: cp.wait_send())


def gather_and_factor(a_t):
    rows = a_t.shape[1]
    width = rows // NC
    vm = lambda *shape: pltpu.VMEM(shape, F32)
    dma = lambda *shape: pltpu.SemaphoreType.DMA(shape)
    out = lambda *shape: jax.ShapeDtypeStruct(shape, F32)
    hbm = pl.BlockSpec(memory_space=pl.ANY)
    scratch = [vm(NP, NC, W, width), vm(NP, W, 256), vm(NP, W, 128), vm(2, W, 128), vm(W, 256), vm(W, 256), vm(W, 256)]
    scratch += [vm(W, 256)]
    scratch += [vm(W, 128)] * 8
    scratch += [vm(NP, 3, W, W), vm(NP, 3, W, W), vm(NP, W, W), vm(NP, W, W), vm(3, W, 384), vm(W, 256), vm(W, 128), vm(8, 256),
                vm(W, 256), vm(W, 256), vm(W, 128), vm(W, 128), vm(NP, W, 256), vm(N, 256), vm(N, 256),
                vm(NP, W), vm(NP, W, W), vm(W, 128), vm(NP, W, W), vm(NP, W, W), vm(8, 128), vm(8, 128), vm(8, 128)]
    scratch += [dma(NC), dma(2, NP, NC), dma(NP, NC), dma(3, 2), dma(3, 2), dma(3, NP), dma(NP), dma(4, NP), dma(3, NP), dma(NP), dma(4, NP),
                dma(3, 2), dma(2), dma(4, 2), dma(2), dma(NP, NC)]
    return pl.pallas_call(
        gather_kernel,
        name="gather_and_factor",
        out_shape=(out(N, rows), out(W, rows), out(AUX_ROWS, 256), out(1)),
        in_specs=[hbm],
        out_specs=(hbm, hbm, pl.BlockSpec(memory_space=pltpu.VMEM), pl.BlockSpec(memory_space=pltpu.SMEM)),
        scratch_shapes=scratch,
        compiler_params=pltpu.CompilerParams(collective_id=0, has_side_effects=True, vmem_limit_bytes=32 * 1024 * 1024),
    )(a_t)


def pack_kernel(tau_ref, t_ref, aux_ref):
    aux_ref[...] = jnp.zeros_like(aux_ref)
    for g in range(NP):
        aux_ref[AUX_T + W * g:AUX_T + W * g + W, 0:W] = t_ref[g]
    aux_ref[AUX_TAU:AUX_TAU + NP, 0:W] = tau_ref[...]
    aux_ref[AUX_MODE:AUX_MODE + 8, :] = jnp.ones((8, 256), F32)


def pack_aux(tau_vals, t_fac):
    return pl.pallas_call(pack_kernel, name="pack_aux", out_shape=jax.ShapeDtypeStruct((AUX_ROWS, 256), F32))(tau_vals, t_fac)


def product_kernel(b_ref, f_alt, aux_ref, q_ref, f_ref, tau_ref, t_ref, sem):
    step = pl.program_id(0)
    width = b_ref.shape[1]
    careful = jnp.max(aux_ref[AUX_MODE:AUX_MODE + 8, 0:128]) > 0.5

    @pl.when(step == 0)
    def _():
        tau_ref[...] = aux_ref[AUX_TAU:AUX_TAU + NP, 0:W]
        for g in range(NP):
            t_ref[g] = aux_ref[AUX_T + W * g:AUX_T + W * g + W, 0:W]

    @pl.when(jnp.logical_not(careful))
    def _():
        prod = mm(aux_ref[0:N + W, 0:N], b_ref[...])
        q_ref[...] = prod[0:N]
        f_ref[...] = prod[N:N + W]

        @pl.when((step == 0) & (lax.axis_index("row") == 0))
        def _():
            keep = iota((W, 256), 1) < N
            f_ref[:, 0:256] = jnp.where(keep, aux_ref[AUX_TOP:AUX_TOP + W, :], prod[N:N + W, 0:256])

    @pl.when(careful)
    def _():
        q_ref[...] = b_ref[...]
        copy = pltpu.make_async_copy(f_alt.at[:, pl.ds(pl.multiple_of(step * width, width), width)], f_ref, sem)
        copy.start()
        copy.wait()


def products(b, f_alt, aux):
    rows = b.shape[1]
    width = rows // STEPS
    out = lambda *shape: jax.ShapeDtypeStruct(shape, F32)
    whole = pl.BlockSpec(memory_space=pltpu.VMEM)
    return pl.pallas_call(
        product_kernel,
        name="products",
        grid=(STEPS,),
        out_shape=(out(N, rows), out(W, rows), out(NP, W), out(NP, W, W)),
        in_specs=[pl.BlockSpec((N, width), lambda i: (0, i)), pl.BlockSpec(memory_space=pl.ANY), whole],
        out_specs=(pl.BlockSpec((N, width), lambda i: (0, i)), pl.BlockSpec((W, width), lambda i: (0, i)), whole, whole),
        scratch_shapes=[pltpu.SemaphoreType.DMA],
        compiler_params=pltpu.CompilerParams(vmem_limit_bytes=32 * 1024 * 1024),
    )(b, f_alt, aux)


def all_pieces(x, axis, n):
    me = lax.axis_index(axis)
    got = jnp.stack([x] + [lax.ppermute(x, axis, [(i, (i + s) % n) for i in range(n)]) for s in range(1, n)])
    return [lax.dynamic_index_in_dim(got, (me - j) % n, axis=0, keepdims=False) for j in range(n)]


def ordered_sum(x, axis, n):
    pieces = all_pieces(x, axis, n)
    total = pieces[0]
    for piece in pieces[1:]:
        total = total + piece
    return total


def dot_high(lhs_mat, rhs_mat):
    return jnp.dot(lhs_mat, rhs_mat, precision=HIGHEST, preferred_element_type=jnp.float32)


def contract(einsum_form, lhs_mat, rhs_mat):
    return jnp.einsum(einsum_form, lhs_mat, rhs_mat, precision=HIGHEST, preferred_element_type=jnp.float32)


def factor_panel(panel_in, row_start, diag0, reduce_rows):
    rows_loc, panel_width = panel_in.shape
    global_rows = row_start + jnp.arange(rows_loc)
    col_ids = jnp.arange(panel_width)

    def column_step(col_step, carried):
        panel_work, refl_vecs, tau_vec = carried
        diag_row = diag0 + col_step
        column = lax.dynamic_index_in_dim(panel_work, col_step, axis=1, keepdims=False)
        x_col = jnp.where(global_rows >= diag_row, column, 0.0)
        local_row = diag_row - row_start
        holds_diag = (local_row >= 0) & (local_row < rows_loc)
        diag_row_vals = lax.dynamic_index_in_dim(panel_work, jnp.clip(local_row, 0, rows_loc - 1), axis=0, keepdims=False)
        diag_piece = jnp.where(holds_diag, diag_row_vals, 0.0)
        summed = reduce_rows(jnp.stack([dot_high(x_col, panel_work), diag_piece]))
        x_dots = summed[0]
        diag_vals = summed[1]
        alpha_val = diag_vals[col_step]
        col_norm = jnp.sqrt(x_dots[col_step])
        beta_val = jnp.where(alpha_val >= 0, -col_norm, col_norm)
        tau_step = (beta_val - alpha_val) / beta_val
        inv_scale = 1.0 / (alpha_val - beta_val)
        at_diag = global_rows == diag_row
        reflector = jnp.where(global_rows > diag_row, x_col * inv_scale, jnp.where(at_diag, 1.0, 0.0))
        v_dots = jnp.where(col_ids > col_step, inv_scale * (x_dots - alpha_val * diag_vals) + diag_vals, 0.0)
        panel_work = panel_work - tau_step * reflector[:, None] * v_dots[None, :]
        new_col = jnp.where(global_rows < diag_row, column, jnp.where(at_diag, beta_val, reflector))
        is_col = col_ids == col_step
        panel_work = jnp.where(is_col[None, :], new_col[:, None], panel_work)
        refl_vecs = jnp.where(is_col[None, :], reflector[:, None], refl_vecs)
        tau_vec = jnp.where(is_col, tau_step, tau_vec)
        return panel_work, refl_vecs, tau_vec

    init_carry = (panel_in, jnp.zeros_like(panel_in), jnp.zeros((panel_width,), jnp.float32))
    return lax.fori_loop(0, panel_width, column_step, init_carry)


def build_tfac(refl_vecs, tau_vec, reduce_rows):
    panel_width = tau_vec.shape[0]
    col_ids = jnp.arange(panel_width)
    gram_mat = reduce_rows(contract("rk,rl->kl", refl_vecs, refl_vecs))

    def t_step(col_step, t_fac):
        g_col = jnp.where(col_ids < col_step, lax.dynamic_index_in_dim(gram_mat, col_step, axis=1, keepdims=False), 0.0)
        tau_step = tau_vec[col_step]
        new_col = jnp.where(col_ids == col_step, tau_step, -tau_step * dot_high(t_fac, g_col))
        return jnp.where(col_ids[None, :] == col_step, new_col[:, None], t_fac)

    return lax.fori_loop(0, panel_width, t_step, jnp.zeros((panel_width, panel_width), jnp.float32))


def careful_program(proc_cols, proc_rows):
    sum_rows = functools.partial(ordered_sum, axis="row", n=proc_rows)

    def local_program(a_loc):
        rows_loc, panels_loc, panel_width = a_loc.shape
        num_panels = panels_loc * proc_cols
        col_idx = lax.axis_index("col")
        row_start = lax.axis_index("row") * rows_loc
        global_rows = row_start + jnp.arange(rows_loc)
        panel_ids = jnp.arange(panels_loc) * proc_cols + col_idx

        def panel_step(panel_idx, carried):
            a_work, all_vecs, all_tfac = carried
            slot_idx = panel_idx // proc_cols
            is_owner = col_idx == panel_idx % proc_cols
            old_panel = lax.dynamic_index_in_dim(a_work, slot_idx, axis=1, keepdims=False)
            new_panel, refl_vecs, tau_vec = factor_panel(old_panel, row_start, panel_idx * panel_width, sum_rows)
            t_fac = build_tfac(refl_vecs, tau_vec, sum_rows)
            refl_vecs = ordered_sum(jnp.where(is_owner, refl_vecs, 0.0), "col", proc_cols)
            t_fac = ordered_sum(jnp.where(is_owner, t_fac, 0.0), "col", proc_cols)
            a_work = lax.dynamic_update_index_in_dim(a_work, jnp.where(is_owner, new_panel, old_panel), slot_idx, axis=1)
            proj_sum = sum_rows(contract("rk,rsj->ksj", refl_vecs, a_work))
            w_block = contract("kl,ksj->lsj", t_fac, proj_sum)
            w_block = jnp.where((panel_ids > panel_idx)[None, :, None], w_block, 0.0)
            a_work = a_work - contract("rl,lsj->rsj", refl_vecs, w_block)
            all_vecs = lax.dynamic_update_index_in_dim(all_vecs, refl_vecs, panel_idx, axis=0)
            all_tfac = lax.dynamic_update_index_in_dim(all_tfac, t_fac, panel_idx, axis=0)
            return a_work, all_vecs, all_tfac

        init_carry = (a_loc, jnp.zeros((num_panels, rows_loc, panel_width), jnp.float32), jnp.zeros((num_panels, panel_width, panel_width), jnp.float32))
        a_work, all_vecs, all_tfac = lax.fori_loop(0, num_panels, panel_step, init_carry)
        logical_cols = panel_ids[:, None] * panel_width + jnp.arange(panel_width)[None, :]
        q_init = (global_rows[:, None, None] == logical_cols[None, :, :]).astype(jnp.float32)

        def q_step(back_step, q_local):
            panel_idx = num_panels - 1 - back_step
            refl_vecs = lax.dynamic_index_in_dim(all_vecs, panel_idx, keepdims=False)
            t_fac = lax.dynamic_index_in_dim(all_tfac, panel_idx, keepdims=False)
            proj_sum = sum_rows(contract("rk,rsj->ksj", refl_vecs, q_local))
            w_block = contract("kl,lsj->ksj", t_fac, proj_sum)
            return q_local - contract("rk,ksj->rsj", refl_vecs, w_block)

        q_local = lax.fori_loop(0, num_panels, q_step, q_init)
        gathered = jnp.stack(all_pieces(q_local, "col", proc_cols))
        q_rows = gathered.transpose(1, 2, 0, 3).reshape(rows_loc, num_panels * panel_width)
        tau_vals = jnp.diagonal(all_tfac, axis1=1, axis2=2)
        return a_work, tau_vals, all_tfac, q_rows

    return local_program


def solution(mesh):
    careful = careful_program(mesh.shape["col"], mesh.shape["row"])

    def local_program(a_loc):
        rows_loc = a_loc.shape[0]
        b, f_alt, aux, flag = gather_and_factor(a_loc.reshape(rows_loc, W).T)

        def again(state):
            factored, tau_new, t_new, q_new = careful(a_loc)
            return jnp.zeros((1,), F32), q_new.T, factored.reshape(rows_loc, W).T, pack_aux(tau_new, t_new)

        b, f_alt, aux = lax.while_loop(lambda s: s[0][0] > 0.5, again, (flag, b, f_alt, aux))[1:]
        q_t, f_t, tau_vals, t_fac = products(b, f_alt, aux)
        return f_t.T.reshape(rows_loc, 1, W), tau_vals, t_fac, q_t.T

    spec_rows = P(("part", "row"), "col", None)
    out_specs = (spec_rows, P("part", None), P("part", None, None), P(("part", "row"), None))
    return jax.shard_map(local_program, mesh=mesh, in_specs=(spec_rows,), out_specs=out_specs, check_vma=False)
```

```python
import functools
import jax
import jax.numpy as jnp
from jax import lax
from jax.experimental import pallas as pl
from jax.experimental.pallas import tpu as pltpu
from jax.sharding import PartitionSpec as P

HIGHEST = lax.Precision.HIGHEST
MESH = pl.DeviceIdType.MESH
W = 48
NP = 4
N = W * NP
NC = 8
WIN = 6
F32 = jnp.float32
SUM_BOUND = 6144.0
HEAD0, HEAD1, HEAD2 = 3, 5, 2
STEPS = 4
EARLY = NC - NC // STEPS
AUX_T = N + W
AUX_TAU = AUX_T + N
AUX_ROWS = AUX_TAU + 8


def mm(a, b):
    return lax.dot_general(a, b, (((1,), (0,)), ((), ())), precision=HIGHEST, preferred_element_type=F32)


def mm_nt(a, b):
    return lax.dot_general(a, b, (((1,), (1,)), ((), ())), precision=HIGHEST, preferred_element_type=F32)


def iota(shape, dim):
    return lax.broadcasted_iota(jnp.int32, shape, dim)


def roll(x, shift):
    shift = shift % x.shape[1]
    return x if shift == 0 else pltpu.roll(x, shift, 1)


def widen(x, lanes):
    return jnp.concatenate([x, jnp.zeros((x.shape[0], lanes - x.shape[1]), F32)], axis=1)


def chain(limit, xc_ref, hn_ref, vt_ref, fr_ref, rn_ref, td_ref, zt_ref):
    ng = W // 8
    sub = iota((8, 128), 0)
    lane = iota((8, 128), 1)
    live0 = lane < limit
    live1 = lane + 128 < limit
    xs0 = [xc_ref[8 * s:8 * s + 8, 0:128] for s in range(ng)]
    xs1 = [xc_ref[8 * s:8 * s + 8, 128:256] for s in range(ng)]
    hs = [hn_ref[8 * s:8 * s + 8, :] for s in range(ng)]
    zs = [jnp.where(lane == sub + 8 * s, 1.0, 0.0) for s in range(ng)]

    def bcast_sub(x, u):
        return jnp.broadcast_to(x[u:u + 1, :], (8, 128))

    def bcast_col(x, k):
        return jnp.broadcast_to(x[:, k:k + 1], (8, 128))

    def columns(k):
        return ({s: bcast_col(hs[s], k) for s in range(k // 8, ng)}, {s: bcast_col(xs0[s], k) for s in range(0, ng)},
                {s: bcast_col(zs[s], k) for s in range(k // 8 + 1)})

    window = {k: columns(k) for k in range(WIN)}
    for k in range(W):
        s0, u = k // 8, k % 8
        ch, cx, cz = window.pop(k)
        hkk = bcast_sub(ch[s0], u)
        alpha = bcast_sub(cx[s0], u)
        inv_norm = lax.rsqrt(hkk)
        inv_beta = jnp.where(alpha >= 0, -inv_norm, inv_norm)
        beta = hkk * inv_beta
        inv = 1.0 / (alpha - beta)
        tau = (beta - alpha) * inv_beta
        below = sub > u
        rc, wc = {}, {}
        for s in range(s0, ng):
            r = ch[s] * inv_beta
            w = cx[s] - r
            rc[s] = jnp.where(below, r, 0.0) if s == s0 else r
            wc[s] = jnp.where(below, w, 0.0) if s == s0 else w
        r_of = {}
        for m in range(k + 1, min(k + WIN, W)):
            mh, mx, mz = window[m]
            r_m = bcast_sub(rc[m // 8], m % 8)
            v_m = bcast_sub(mx[s0], u) * inv
            for s in range(m // 8, ng):
                mh[s] = mh[s] - rc[s] * r_m
            for s in range(s0, ng):
                mx[s] = mx[s] - wc[s] * v_m
            for s in range(s0 + 1):
                mz[s] = mz[s] - cz[s] * v_m
        hrow = bcast_sub(hs[s0], u) * inv_beta
        x0 = bcast_sub(xs0[s0], u)
        x1 = bcast_sub(xs1[s0], u)
        s0v = x0 * inv
        v0 = jnp.where(live0 & (lane > k), s0v, jnp.where(lane == k, 1.0, 0.0))
        v1 = jnp.where(live1, x1 * inv, 0.0)
        vt_ref[k:k + 1, 0:128] = v0[0:1, :]
        vt_ref[k:k + 1, 128:256] = v1[0:1, :]
        fr_ref[k:k + 1, 0:128] = jnp.where(live0 & (lane > k), s0v, jnp.where(lane == k, beta, x0))[0:1, :]
        fr_ref[k:k + 1, 128:256] = jnp.where(live1, v1, x1)[0:1, :]
        rn_ref[k:k + 1, :] = hrow[0:1, :]
        td_ref[k:k + 1, :] = jnp.where(lane == k, tau, 0.0)[0:1, :]
        for s in range(s0, ng):
            hs[s] = hs[s] - rc[s] * hrow
            xs0[s] = xs0[s] - wc[s] * v0
            xs1[s] = xs1[s] - wc[s] * v1
        v_next = jnp.where(lane == k, 0.0, v0)
        for s in range(s0 + 1):
            zs[s] = zs[s] - cz[s] * v_next
        if k + WIN < W:
            window[k + WIN] = columns(k + WIN)
    for s in range(ng):
        zt_ref[8 * s:8 * s + 8, :] = zs[s]


def load_panel(g, refs):
    xt, e1, e2, rts, wts, rinvd, kvt, xc_ref, hn_ref, dvec = (
        refs["xt"], refs["e1"], refs["e2"], refs["rts"], refs["wts"], refs["rinvd"], refs["kv"], refs["xc"], refs["hn"], refs["dvec"])
    x = xt[g]
    lane = iota((W, 256), 1)
    row = iota((W, 256), 0)
    diag = jnp.sum(jnp.where(lane == row + N, x, 0.0), axis=0, keepdims=True)
    dvec[0:1, :] = dvec[0:1, :] + roll(diag, 64 + W * g)
    gram = roll(x, 64)[:, 0:128]
    lane1 = lane[:, 0:128]
    row1 = row[:, 0:128]
    x = jnp.where(lane >= N, jnp.where(lane == row + N, 1.0, 0.0), x)
    hgg = gram[:, 0:W]
    for h in range(g):
        if g - h == 1:
            hgh = e1[g][:, 0:W]
        elif g - h == 2:
            hgh = roll(e1[g], 80)[:, 0:W]
        else:
            hgh = e2[0][:, 0:W] + e2[1][:, 0:W]
        for q in range(h):
            hgh = hgh - mm_nt(rts[g, q], rts[h, q])
        rt = mm_nt(hgh, rinvd[h])
        both = mm(x[:, 0:W] - rt, kvt[h])
        x = roll(x - both[:, 0:256], 256 - W)
        hgg = hgg - mm_nt(rt, rt)
        rts[g, h] = rt
        wts[g, h] = both[:, 256:256 + W]
    xc_ref[...] = x
    hn_ref[...] = jnp.where(lane1 < W, widen(hgg, 128), jnp.where(lane1 == row1 + 64, 1.0, 0.0))


def close_panel(g, refs):
    vt = refs["vt"][...]
    fr = refs["fr"][...]
    rn = refs["rn"][...]
    td = refs["td"][...]
    lane = iota((W, 256), 1)
    lane1 = iota((W, 128), 1)
    row1 = iota((W, 128), 0)
    sq_lane = iota((W, W), 1)
    sq_row = iota((W, W), 0)
    refs["ftop"][g] = roll(fr, W * g)
    mt = roll(vt, 64 + W * g)[:, 0:W]
    v = jnp.where(lane < N - W * g, vt, 0.0)
    rnat = jnp.where((lane1 >= row1) & (lane1 < W), rn, 0.0)[:, 0:W]
    rinvt = roll(rn, 64)[:, 0:W]
    rinvt = jnp.where(sq_lane <= sq_row, rinvt, 0.0)
    mt = jnp.where(sq_lane <= sq_row, mt, 0.0)
    refs["rinvd"][g] = rinvt
    refs["rnat"][g] = rnat
    refs["mts"][g] = mt
    refs["v1"][g] = v[:, 0:W]
    refs["t"][g] = td[:, 0:W]
    refs["tau"][g:g + 1, :] = jnp.sum(td, axis=0, keepdims=True)[:, 0:W]
    zt = refs["zt"][:, 0:W]
    refs["zsum"][...] = refs["zsum"][...] + jnp.sum(zt * zt)
    if g + 1 < NP:
        refs["kv"][g, :, 0:256] = mm(zt, v)
        refs["kv"][g, :, 256:384] = widen(zt, 128)
    lr = roll(widen(rinvt, 256), W * g)
    lc = roll(widen(mt, 256), W * g)
    if g:
        rcat = sum(roll(widen(refs["rts"][g, h], 256), W * h) for h in range(g))
        wcat = sum(roll(widen(refs["wts"][g, h], 256), W * h) for h in range(g))
        lr = lr - mm(mm(rinvt, rcat)[:, 0:N], refs["lr"][...])
        lc = lc - mm(mm(mt, wcat)[:, 0:N], refs["lc"][...])
    refs["lr"][W * g:W * g + W, :] = lr
    refs["lc"][W * g:W * g + W, :] = lc


def build_t(refs):
    sq_lane = iota((W, W), 1)
    sq_row = iota((W, W), 0)
    prods = [mm_nt(refs["rnat"][g], refs["mts"][g]) for g in range(NP)]
    ss = [-mm(refs["v1"][g], prods[g]) for g in range(NP)]
    ts = [refs["t"][g] for g in range(NP)]
    size = 1
    while size < W:
        pair = (sq_row // (2 * size) == sq_lane // (2 * size)) & (sq_row // size < sq_lane // size)
        halves = [mm(ts[g], jnp.where(pair, ss[g], 0.0)) for g in range(NP)]
        ts = [ts[g] - mm(halves[g], ts[g]) for g in range(NP)]
        size *= 2
    for g in range(NP):
        refs["t"][g] = ts[g]


def gather_kernel(a_hbm, b_ref, f_alt, aux_ref, flag_ref, panels, xt, e1, e2, x0s, x1s, x2s, x3s, g1s, g1r, g2s, g2r, h1s, h1r, h2s, h2r,
                 rts, wts, rinvd, rnat, kvt, xc, hn, dvec, vt, fr, rn, td, ftop, lr, lc, tau, t_fac, zt, mts, v1s, zsum, bad_mine, bad_other,
                 load_sem, send_sem, bulk_sem, ex_send, ex_recv, e0_send, e0_recv, e0_row, e1_send, e1_recv, e1_row, e2_send, e2_recv, e2_row, flag_sem):
    refs = dict(xt=xt, e1=e1, e2=e2, rts=rts, wts=wts, rinvd=rinvd, rnat=rnat, kv=kvt, xc=xc, hn=hn, dvec=dvec,
                vt=vt, fr=fr, rn=rn, td=td, ftop=ftop, lr=lr, lc=lc, tau=tau, t=t_fac, zt=zt, mts=mts, v1=v1s, zsum=zsum)
    part = lax.axis_index("part")
    c = lax.axis_index("col")
    r = lax.axis_index("row")
    width = panels.shape[3]
    twin = r + 1 - 2 * lax.rem(r, 2)
    across = lax.rem(r + 2, 4)

    def at(col, row):
        return (part, col, row)

    for q in range(NC):
        pltpu.make_async_copy(a_hbm.at[:, pl.ds(q * width, width)], panels.at[c, q], load_sem.at[q]).start()

    barrier = pltpu.get_barrier_semaphore()
    peers = [at(lax.rem(c + s, NP), r) for s in range(1, NP)] + [at(c, twin), at(c, across), (1 - part, c, r)]
    for peer in peers:
        pl.semaphore_signal(barrier, inc=1, device_id=peer, device_id_type=MESH)
    pl.semaphore_wait(barrier, len(peers))

    lr[...] = jnp.zeros_like(lr)
    lc[...] = jnp.zeros_like(lc)
    dvec[...] = jnp.zeros_like(dvec)
    zsum[...] = jnp.zeros_like(zsum)
    e2[...] = jnp.zeros_like(e2)

    order_load = [q for i in range(NC // 2) for q in (i, i + NC // 2)]
    order_l = list(range(NC))
    order_r = list(range(NC // 2, NC)) + list(range(NC // 2))

    def bulk(side, g, q):
        other = c - 1 if side == 0 else c + 1
        return pltpu.make_async_remote_copy(
            src_ref=panels.at[g, q], dst_ref=panels.at[g, q], send_sem=send_sem.at[side, g, q], recv_sem=bulk_sem.at[g, q],
            device_id=at(other, r), device_id_type=MESH)

    def start_own(i):
        @pl.when(c >= 1)
        def _():
            bulk(0, c, order_l[i]).start()

        @pl.when(c <= NP - 2)
        def _():
            bulk(1, c, order_r[i]).start()

    def arrive(dist, i):
        @pl.when(c + dist <= NP - 1)
        def _():
            bulk(0, c + dist, order_l[i]).wait_recv()

        @pl.when(c - dist >= 0)
        def _():
            bulk(1, c - dist, order_r[i]).wait_recv()

    def forward(dist, i):
        @pl.when((c + dist <= NP - 1) & (c >= 1))
        def _():
            bulk(0, c + dist, order_l[i]).start()

        @pl.when((c - dist >= 0) & (c <= NP - 2))
        def _():
            bulk(1, c - dist, order_r[i]).start()

    def row_sum(e, mine, got1, half, got2, out, slot):
        first = pltpu.make_async_remote_copy(mine, got1, ex_send.at[e, 0], ex_recv.at[e, 0], device_id=at(c, twin), device_id_type=MESH)
        first.start()
        first.wait()
        half[...] = mine[...] + got1[...]
        second = pltpu.make_async_remote_copy(half, got2, ex_send.at[e, 1], ex_recv.at[e, 1], device_id=at(c, across), device_id_type=MESH)
        second.start()
        second.wait()
        out[slot] = half[...] + got2[...]

    rows_mine = pl.ds(pl.multiple_of(lax.rem(r, 2) * (W // 2), 8), W // 2)
    lanes_mine = pl.ds(pl.multiple_of(lax.div(r, 2) * 128, 128), 128)

    class Message:
        def __init__(self, ref, slot, sems, quarter, source):
            self.ref, self.slot, self.sems, self.quarter, self.source = ref, slot, sems, quarter, source

        def copy(self, ref, send, recv, peer):
            return pltpu.make_async_remote_copy(ref, ref, send, recv, device_id=peer, device_id_type=MESH)

        def hop(self, s):
            part_ref = self.ref.at[self.slot, rows_mine, lanes_mine] if self.quarter else self.ref.at[self.slot, rows_mine]
            return self.copy(part_ref, self.sems[0].at[s - 1, self.slot], self.sems[1].at[self.slot], at(lax.rem(c + s, NP), r))

        def to_twin(self):
            part_ref = self.ref.at[self.slot, rows_mine, lanes_mine] if self.quarter else self.ref.at[self.slot, rows_mine]
            return self.copy(part_ref, self.sems[2].at[0, self.slot], self.sems[2].at[1, self.slot], at(c, twin))

        def to_across(self):
            return self.copy(self.ref.at[self.slot, :, lanes_mine], self.sems[2].at[2, self.slot], self.sems[2].at[3, self.slot], at(c, across))

        def each_hop(self, act):
            @pl.when(c == self.source)
            def _():
                for s in range(1, NP):
                    act(self.hop(s))

        def send_on(self):
            self.each_hop(lambda cp: cp.start())

        def receive(self):
            @pl.when(c != self.source)
            def _():
                self.hop(1).wait_recv()
                self.to_twin().start()

        def join(self):
            @pl.when(c != self.source)
            def _():
                self.to_twin().wait()
                if self.quarter:
                    self.to_across().start()

        def finish(self):
            if self.quarter:
                @pl.when(c != self.source)
                def _():
                    self.to_across().wait()

    msg0 = [Message(xt, g, (e0_send, e0_recv, e0_row), True, g) for g in range(NP)]
    msg1 = [None] + [Message(e1, g, (e1_send, e1_recv, e1_row), False, g - 1) for g in range(1, NP)]
    msg2 = [Message(e2, i, (e2_send, e2_recv, e2_row), False, i + 1) for i in range(2)]

    def take(messages):
        for m in messages:
            m.receive()
        for m in messages:
            m.join()
        for m in messages:
            m.finish()

    def chunk_cols(g, q):
        return panels[g, q]

    started = 0
    for q in range(NC):
        pltpu.make_async_copy(a_hbm.at[:, pl.ds(order_load[q] * width, width)], panels.at[c, order_load[q]], load_sem.at[order_load[q]]).wait()
        if q % 2 and started < HEAD0:
            start_own(started)
            started += 1
    gram = jnp.zeros((W, W), F32)
    for q in range(NC):
        blk = chunk_cols(c, q)
        gram = gram + mm_nt(blk, blk)
    lane = iota((W, 256), 1)
    top = jnp.where((lane < N) & (r == 0), panels[c, 0, :, 0:256], 0.0)
    x0s[...] = top + roll(widen(gram, 256), N)
    row_sum(0, x0s, x1s, x2s, x3s, xt, c)
    for m in msg0:
        m.send_on()
    for i in range(started, NC):
        start_own(i)

    def before(g):
        if g == 0:
            take(msg0)
        if g == 1:
            g1s[...] = jnp.zeros_like(g1s)
            left = jnp.maximum(c - 1, 0)
            for i in range(NC):
                arrive(1, i)
                if i < HEAD1:
                    forward(1, i)

                @pl.when(c <= NP - 2)
                def _():
                    for q in ([i, i - NC // 2] if i >= NC // 2 else []):
                        pair = jnp.concatenate([chunk_cols(c, q), chunk_cols(left, q)], axis=0)
                        g1s[:, 0:2 * W] += mm_nt(chunk_cols(c + 1, q), pair)

            @pl.when(c <= NP - 2)
            def _():
                row_sum(1, g1s, g1r, g2s, g2r, e1, c + 1)
            for m in msg1[1:]:
                m.send_on()
            for i in range(HEAD1, NC):
                forward(1, i)
            half = NC // 2
            for i in range(half):
                arrive(2, i)
                if i < HEAD2:
                    forward(2, i)

            @pl.when((c >= 1) & (c <= 2))
            def _():
                base = (c - 1) * half
                acc = jnp.zeros((W, W), F32)
                for i in range(half):
                    acc = acc + mm_nt(chunk_cols(3, base + i), chunk_cols(0, base + i))
                h1s[...] = widen(acc, 128)
                row_sum(2, h1s, h1r, h2s, h2r, e2, c - 1)
            for m in msg2:
                m.send_on()
            for i in range(HEAD2, half):
                forward(2, i)
            take(msg1[1:])
        if g == 2:
            for i in range(NC // 2, NC):
                arrive(2, i)
                forward(2, i)
        if g == 3:
            take(msg2)

    def panel_step(g, carry):
        for s in range(NP):
            @pl.when(g == s)
            def _():
                before(s)
                load_panel(s, refs)
        chain(256 - W * g, xc, hn, vt, fr, rn, td, zt)
        for s in range(NP):
            @pl.when(g == s)
            def _():
                close_panel(s, refs)
        return carry

    lax.fori_loop(0, NP, panel_step, 0)

    dv = dvec[0:1, 0:N]
    lr_all = lr[...][:, 0:N]
    lc_all = lc[...][:, 0:N]
    good = ((jnp.sum(lr_all * lr_all * dv) <= SUM_BOUND) & (jnp.sum(lc_all * lc_all * dv) <= SUM_BOUND)
            & (jnp.max(zsum[...]) <= SUM_BOUND) & (jnp.min(dv) > 1e-18) & (jnp.max(dv) < 1e30))
    bad_mine[...] = jnp.zeros((8, 128), F32) + jnp.where(good, 0.0, 1.0)
    flag_copy = pltpu.make_async_remote_copy(bad_mine, bad_other, flag_sem.at[0], flag_sem.at[1], device_id=(1 - part, c, r), device_id_type=MESH)
    flag_copy.start()
    build_t(refs)

    aux_ref[0:N, :] = lr[...]
    aux_ref[N:N + W, :] = lc[pl.ds(pl.multiple_of(c * W, W), W), :]
    for g in range(NP):
        aux_ref[AUX_T + W * g:AUX_T + W * g + W, :] = widen(t_fac[g], 256)
    aux_ref[AUX_TAU:AUX_TAU + 8, :] = jnp.concatenate([widen(tau[...], 256), jnp.zeros((4, 256), F32)], axis=0)

    ftop_c = ftop[c]
    for i in range(NC):
        arrive(3, i)
        q = lax.rem(i + jnp.where(c >= NP // 2, NC // 2, 0), NC)
        cols = pl.ds(pl.multiple_of(q * width, width), width)
        if i < EARLY:
            prod = mm(aux_ref[0:N + W, 0:N], jnp.concatenate([panels[g, q] for g in range(NP)], axis=0))
            b_ref[:, cols] = prod[0:N]
            f_alt[:, cols] = prod[N:N + W]

            @pl.when((q == 0) & (r == 0))
            def _():
                keep = iota((W, 256), 1) < N
                f_alt[:, 0:256] = jnp.where(keep, ftop_c, prod[N:N + W, 0:256])
        else:
            for g in range(NP):
                b_ref[g * W:g * W + W, cols] = panels[g, q]
    flag_copy.wait()
    flag_ref[0] = jnp.max(jnp.maximum(bad_mine[...], bad_other[...]))

    for i in range(NC):
        @pl.when(c >= 1)
        def _():
            for s in range(NP):
                @pl.when(c <= s)
                def _():
                    bulk(0, s, i).wait_send()

        @pl.when(c <= NP - 2)
        def _():
            for s in range(NP):
                @pl.when(c >= s)
                def _():
                    bulk(1, s, i).wait_send()
    for m in msg0 + msg1[1:] + msg2:
        m.each_hop(lambda cp: cp.wait_send())


def gather_and_factor(a_t):
    rows = a_t.shape[1]
    width = rows // NC
    vm = lambda *shape: pltpu.VMEM(shape, F32)
    dma = lambda *shape: pltpu.SemaphoreType.DMA(shape)
    out = lambda *shape: jax.ShapeDtypeStruct(shape, F32)
    hbm = pl.BlockSpec(memory_space=pl.ANY)
    vmem = pl.BlockSpec(memory_space=pltpu.VMEM)
    scratch = [vm(NP, NC, W, width), vm(NP, W, 256), vm(NP, W, 128), vm(2, W, 128), vm(W, 256), vm(W, 256), vm(W, 256)]
    scratch += [vm(W, 256)]
    scratch += [vm(W, 128)] * 8
    scratch += [vm(NP, 3, W, W), vm(NP, 3, W, W), vm(NP, W, W), vm(NP, W, W), vm(3, W, 384), vm(W, 256), vm(W, 128), vm(8, 256),
                vm(W, 256), vm(W, 256), vm(W, 128), vm(W, 128), vm(NP, W, 256), vm(N, 256), vm(N, 256),
                vm(NP, W), vm(NP, W, W), vm(W, 128), vm(NP, W, W), vm(NP, W, W), vm(8, 128), vm(8, 128), vm(8, 128)]
    scratch += [dma(NC), dma(2, NP, NC), dma(NP, NC), dma(3, 2), dma(3, 2), dma(3, NP), dma(NP), dma(4, NP), dma(3, NP), dma(NP), dma(4, NP),
                dma(3, 2), dma(2), dma(4, 2), dma(2)]
    return pl.pallas_call(
        gather_kernel,
        name="gather_and_factor",
        out_shape=(out(N, rows), out(W, rows), out(AUX_ROWS, 256), out(1)),
        in_specs=[hbm],
        out_specs=(vmem, vmem, vmem, pl.BlockSpec(memory_space=pltpu.SMEM)),
        scratch_shapes=scratch,
        compiler_params=pltpu.CompilerParams(collective_id=0, has_side_effects=True, vmem_limit_bytes=32 * 1024 * 1024),
    )(a_t)


def product_kernel(b_ref, f_alt, aux_ref, q_hbm, f_hbm, tau_ref, t_ref, q_late, f_late, sems):
    width = q_late.shape[1]

    def out(block, q_src, f_src):
        cols = pl.ds(pl.multiple_of(block * width, width), width)
        return (pltpu.make_async_copy(q_src, q_hbm.at[:, cols], sems.at[0, block]),
                pltpu.make_async_copy(f_src, f_hbm.at[:, cols], sems.at[1, block]))

    late = jnp.where(lax.axis_index("col") >= NP // 2, STEPS // 2 - 1, STEPS - 1)

    def each_early(act):
        for i in range(1, STEPS):
            block = lax.rem(late + i, STEPS)
            cols = pl.ds(pl.multiple_of(block * width, width), width)
            for cp in out(block, b_ref.at[:, cols], f_alt.at[:, cols]):
                act(cp)

    each_early(lambda cp: cp.start())
    tau_ref[...] = aux_ref[AUX_TAU:AUX_TAU + NP, 0:W]
    for g in range(NP):
        t_ref[g] = aux_ref[AUX_T + W * g:AUX_T + W * g + W, 0:W]
    half = width // 2
    for i in range(2):
        prod = mm(aux_ref[0:N + W, 0:N], b_ref[:, pl.ds(pl.multiple_of(late * width + i * half, half), half)])
        q_late[:, i * half:i * half + half] = prod[0:N]
        f_late[:, i * half:i * half + half] = prod[N:N + W]
    last = out(late, q_late, f_late)
    for cp in last:
        cp.start()
    each_early(lambda cp: cp.wait())
    for cp in last:
        cp.wait()


def products(b, f_alt, aux):
    rows = b.shape[1]
    width = rows // STEPS
    out = lambda *shape: jax.ShapeDtypeStruct(shape, F32)
    whole = pl.BlockSpec(memory_space=pltpu.VMEM)
    hbm = pl.BlockSpec(memory_space=pl.ANY)
    return pl.pallas_call(
        product_kernel,
        name="products",
        out_shape=(out(N, rows), out(W, rows), out(NP, W), out(NP, W, W)),
        in_specs=[whole, whole, whole],
        out_specs=(hbm, hbm, whole, whole),
        scratch_shapes=[pltpu.VMEM((N, width), F32), pltpu.VMEM((W, width), F32), pltpu.SemaphoreType.DMA((2, STEPS))],
        compiler_params=pltpu.CompilerParams(vmem_limit_bytes=32 * 1024 * 1024),
    )(b, f_alt, aux)


def same_kernel(tau_in, t_in, tau_ref, t_ref):
    tau_ref[...] = tau_in[...]
    t_ref[...] = t_in[...]


def row_major(tau_vals, t_fac):
    out = lambda x: jax.ShapeDtypeStruct(x.shape, F32)
    return pl.pallas_call(same_kernel, name="row_major", out_shape=(out(tau_vals), out(t_fac)))(tau_vals, t_fac)


def all_pieces(x, axis, n):
    me = lax.axis_index(axis)
    got = jnp.stack([x] + [lax.ppermute(x, axis, [(i, (i + s) % n) for i in range(n)]) for s in range(1, n)])
    return [lax.dynamic_index_in_dim(got, (me - j) % n, axis=0, keepdims=False) for j in range(n)]


def ordered_sum(x, axis, n):
    pieces = all_pieces(x, axis, n)
    total = pieces[0]
    for piece in pieces[1:]:
        total = total + piece
    return total


def dot_high(lhs_mat, rhs_mat):
    return jnp.dot(lhs_mat, rhs_mat, precision=HIGHEST, preferred_element_type=jnp.float32)


def contract(einsum_form, lhs_mat, rhs_mat):
    return jnp.einsum(einsum_form, lhs_mat, rhs_mat, precision=HIGHEST, preferred_element_type=jnp.float32)


def factor_panel(panel_in, row_start, diag0, reduce_rows):
    rows_loc, panel_width = panel_in.shape
    global_rows = row_start + jnp.arange(rows_loc)
    col_ids = jnp.arange(panel_width)

    def column_step(col_step, carried):
        panel_work, refl_vecs, tau_vec = carried
        diag_row = diag0 + col_step
        column = lax.dynamic_index_in_dim(panel_work, col_step, axis=1, keepdims=False)
        x_col = jnp.where(global_rows >= diag_row, column, 0.0)
        local_row = diag_row - row_start
        holds_diag = (local_row >= 0) & (local_row < rows_loc)
        diag_row_vals = lax.dynamic_index_in_dim(panel_work, jnp.clip(local_row, 0, rows_loc - 1), axis=0, keepdims=False)
        diag_piece = jnp.where(holds_diag, diag_row_vals, 0.0)
        summed = reduce_rows(jnp.stack([dot_high(x_col, panel_work), diag_piece]))
        x_dots = summed[0]
        diag_vals = summed[1]
        alpha_val = diag_vals[col_step]
        col_norm = jnp.sqrt(x_dots[col_step])
        beta_val = jnp.where(alpha_val >= 0, -col_norm, col_norm)
        tau_step = (beta_val - alpha_val) / beta_val
        inv_scale = 1.0 / (alpha_val - beta_val)
        at_diag = global_rows == diag_row
        reflector = jnp.where(global_rows > diag_row, x_col * inv_scale, jnp.where(at_diag, 1.0, 0.0))
        v_dots = jnp.where(col_ids > col_step, inv_scale * (x_dots - alpha_val * diag_vals) + diag_vals, 0.0)
        panel_work = panel_work - tau_step * reflector[:, None] * v_dots[None, :]
        new_col = jnp.where(global_rows < diag_row, column, jnp.where(at_diag, beta_val, reflector))
        is_col = col_ids == col_step
        panel_work = jnp.where(is_col[None, :], new_col[:, None], panel_work)
        refl_vecs = jnp.where(is_col[None, :], reflector[:, None], refl_vecs)
        tau_vec = jnp.where(is_col, tau_step, tau_vec)
        return panel_work, refl_vecs, tau_vec

    init_carry = (panel_in, jnp.zeros_like(panel_in), jnp.zeros((panel_width,), jnp.float32))
    return lax.fori_loop(0, panel_width, column_step, init_carry)


def build_tfac(refl_vecs, tau_vec, reduce_rows):
    panel_width = tau_vec.shape[0]
    col_ids = jnp.arange(panel_width)
    gram_mat = reduce_rows(contract("rk,rl->kl", refl_vecs, refl_vecs))

    def t_step(col_step, t_fac):
        g_col = jnp.where(col_ids < col_step, lax.dynamic_index_in_dim(gram_mat, col_step, axis=1, keepdims=False), 0.0)
        tau_step = tau_vec[col_step]
        new_col = jnp.where(col_ids == col_step, tau_step, -tau_step * dot_high(t_fac, g_col))
        return jnp.where(col_ids[None, :] == col_step, new_col[:, None], t_fac)

    return lax.fori_loop(0, panel_width, t_step, jnp.zeros((panel_width, panel_width), jnp.float32))


def careful_program(proc_cols, proc_rows):
    sum_rows = functools.partial(ordered_sum, axis="row", n=proc_rows)

    def local_program(a_loc):
        rows_loc, panels_loc, panel_width = a_loc.shape
        num_panels = panels_loc * proc_cols
        col_idx = lax.axis_index("col")
        row_start = lax.axis_index("row") * rows_loc
        global_rows = row_start + jnp.arange(rows_loc)
        panel_ids = jnp.arange(panels_loc) * proc_cols + col_idx

        def panel_step(panel_idx, carried):
            a_work, all_vecs, all_tfac = carried
            slot_idx = panel_idx // proc_cols
            is_owner = col_idx == panel_idx % proc_cols
            old_panel = lax.dynamic_index_in_dim(a_work, slot_idx, axis=1, keepdims=False)
            new_panel, refl_vecs, tau_vec = factor_panel(old_panel, row_start, panel_idx * panel_width, sum_rows)
            t_fac = build_tfac(refl_vecs, tau_vec, sum_rows)
            refl_vecs = ordered_sum(jnp.where(is_owner, refl_vecs, 0.0), "col", proc_cols)
            t_fac = ordered_sum(jnp.where(is_owner, t_fac, 0.0), "col", proc_cols)
            a_work = lax.dynamic_update_index_in_dim(a_work, jnp.where(is_owner, new_panel, old_panel), slot_idx, axis=1)
            proj_sum = sum_rows(contract("rk,rsj->ksj", refl_vecs, a_work))
            w_block = contract("kl,ksj->lsj", t_fac, proj_sum)
            w_block = jnp.where((panel_ids > panel_idx)[None, :, None], w_block, 0.0)
            a_work = a_work - contract("rl,lsj->rsj", refl_vecs, w_block)
            all_vecs = lax.dynamic_update_index_in_dim(all_vecs, refl_vecs, panel_idx, axis=0)
            all_tfac = lax.dynamic_update_index_in_dim(all_tfac, t_fac, panel_idx, axis=0)
            return a_work, all_vecs, all_tfac

        init_carry = (a_loc, jnp.zeros((num_panels, rows_loc, panel_width), jnp.float32), jnp.zeros((num_panels, panel_width, panel_width), jnp.float32))
        a_work, all_vecs, all_tfac = lax.fori_loop(0, num_panels, panel_step, init_carry)
        logical_cols = panel_ids[:, None] * panel_width + jnp.arange(panel_width)[None, :]
        q_init = (global_rows[:, None, None] == logical_cols[None, :, :]).astype(jnp.float32)

        def q_step(back_step, q_local):
            panel_idx = num_panels - 1 - back_step
            refl_vecs = lax.dynamic_index_in_dim(all_vecs, panel_idx, keepdims=False)
            t_fac = lax.dynamic_index_in_dim(all_tfac, panel_idx, keepdims=False)
            proj_sum = sum_rows(contract("rk,rsj->ksj", refl_vecs, q_local))
            w_block = contract("kl,lsj->ksj", t_fac, proj_sum)
            return q_local - contract("rk,ksj->rsj", refl_vecs, w_block)

        q_local = lax.fori_loop(0, num_panels, q_step, q_init)
        gathered = jnp.stack(all_pieces(q_local, "col", proc_cols))
        q_rows = gathered.transpose(1, 2, 0, 3).reshape(rows_loc, num_panels * panel_width)
        tau_vals = jnp.diagonal(all_tfac, axis1=1, axis2=2)
        return a_work, tau_vals, all_tfac, q_rows

    return local_program


def solution(mesh):
    careful = careful_program(mesh.shape["col"], mesh.shape["row"])

    def local_program(a_loc):
        rows_loc = a_loc.shape[0]
        b, f_alt, aux, flag = gather_and_factor(a_loc.reshape(rows_loc, W).T)

        def again(state):
            factored, tau_new, t_new, q_new = careful(a_loc)
            tau_new, t_new = row_major(tau_new, t_new)
            return jnp.zeros((1,), F32), q_new.T, factored.reshape(rows_loc, W).T, tau_new, t_new

        state = (flag,) + tuple(products(b, f_alt, aux))
        q_t, f_t, tau_vals, t_fac = lax.while_loop(lambda s: s[0][0] > 0.5, again, state)[1:]
        return f_t.T.reshape(rows_loc, 1, W), tau_vals, t_fac, q_t.T

    spec_rows = P(("part", "row"), "col", None)
    out_specs = (spec_rows, P("part", None), P("part", None, None), P(("part", "row"), None))
    return jax.shard_map(local_program, mesh=mesh, in_specs=(spec_rows,), out_specs=out_specs, check_vma=False)
```
